32 devices in a mesh: dp: 2 (over core), gx: 4 (over y, x), gy: 4 (over z).
Axes of the slice: x: 2, y: 2, z: 4, core: 2. Of those that a mesh axis runs over, the one named last changes fastest.
Arguments:
- volume: bfloat16 [2, 4, 8, 32, 128], P('dp', None, 'gx', 'gy'), may hold values from -6 to 6
- targets: float32 [2, 4], P('dp'), may hold values from -4 to 4
- conv1_w: bfloat16 [27, 128], replicated, may hold values from -0.625 to 0.625
- conv1_b: float32 [32], replicated, may hold values from -3 to 3
- conv2_w: bfloat16 [27, 2048], replicated, may hold values from -0.21875 to 0.21875
- conv2_b: float32 [64], replicated, may hold values from -3 to 3
- head_w: float32 [64, 4], replicated, may hold values from -2 to 2
- head_b: float32 [4], replicated, may hold values from -4 to 4
- dir1: float32 [27, 128], replicated, may hold values from -6 to 6
- dir2: float32 [27, 2048], replicated, may hold values from -1.2 to 1.2
- dir_head: float32 [64, 4], replicated, may hold values from -6 to 6
Outputs:
- next1: float32 [27, 128], replicated
- next2: float32 [27, 2048], replicated
- next_head: float32 [64, 4], replicated
- rayleigh: float32 [], replicated
- curvature_field: float32 [2, 32, 8, 32, 128], P('dp', None, 'gx', 'gy')
The draws below stay inside these ranges and needn't reach their ends.
All inputs are finite; a program needn't handle non-finite values.
Results may differ from the reference program's by a relative error of at most 0.0051.
Values may be sent and summed in bfloat16 or wider, within the bound.
A program may use at most 128 MiB of HBM per device.

```python
import jax
import jax.numpy as jnp
from jax import lax

C0 = 4
C1 = 32
C2 = 64
OUT = 4
BATCH = 2
NX = 8
NY = 32
NZ = 128


def block_scale(stream_key, extent, cuts, smallest, top_value):
    def one(dim, parts):
        draws = jax.random.uniform(jax.random.fold_in(jax.random.fold_in(stream_key, 6), dim), (parts,), jnp.float32, smallest / len(cuts), top_value / len(cuts))
        return jnp.repeat(jnp.exp(draws), extent[dim] // parts).reshape((-1,) + (1,) * (len(extent) - dim - 1))

    gain = one(*cuts[0])
    for cut in cuts[1:]:
        gain = gain * one(*cut)
    return gain


def gaussian(rng, extent, scale, reach, cuts=(), dtype=jnp.bfloat16):
    factor_of = block_scale(rng, extent, cuts, -0.22, 0.18) if cuts else 1.0
    entries = jax.random.normal(rng, extent, jnp.float32) * scale * factor_of
    return jnp.minimum(jnp.maximum(entries, -reach), reach).astype(dtype)


def setup_inputs(seed: int = 0) -> dict:
    keys = jax.random.split(jax.random.key(seed), 12)
    volume = gaussian(keys[0], (BATCH, C0, NX, NY, NZ), 1.0, 6.0, ((0, 2), (2, 4), (3, 4)))
    targets = gaussian(keys[1], (BATCH, OUT), 1.0, 4.0, ((0, 2),), jnp.float32)
    conv1_w = gaussian(keys[2], (27, C1 * C0), (27 * C0) ** -0.5, 0.625)
    conv1_b = gaussian(keys[3], (C1,), 0.5, 3.0, (), jnp.float32)
    conv2_w = gaussian(keys[4], (27, C2 * C1), (27 * C1) ** -0.5, 0.21875)
    conv2_b = gaussian(keys[5], (C2,), 0.5, 3.0, (), jnp.float32)
    head_w = gaussian(keys[6], (C2, OUT), (C2 // 8) ** -0.5, 2.0, (), jnp.float32)
    head_b = gaussian(keys[7], (OUT,), 1.0, 4.0, (), jnp.float32)
    dir1 = gaussian(keys[8], (27, C1 * C0), 1.0, 6.0, (), jnp.float32)
    dir2 = gaussian(keys[9], (27, C2 * C1), 0.2, 1.2, (), jnp.float32)
    dir_head = gaussian(keys[10], (C2, OUT), 1.0, 6.0, (), jnp.float32)
    return dict(volume=volume, targets=targets, conv1_w=conv1_w, conv1_b=conv1_b, conv2_w=conv2_w, conv2_b=conv2_b, head_w=head_w, head_b=head_b, dir1=dir1, dir2=dir2, dir_head=dir_head)


def silu_parts(z):
    s = jax.nn.sigmoid(z)
    return (z * s, s * (1.0 + z * (1.0 - s)), s * (1.0 - s) * (2.0 + z * (1.0 - 2.0 * s)))

def as_kernel(flat, outer, inner):
    return flat.reshape(3, 3, 3, outer, inner).transpose(3, 4, 0, 1, 2)

def as_flat(kernel):
    return kernel.transpose(2, 3, 4, 0, 1).reshape(27, kernel.shape[0] * kernel.shape[1])

def pad_plane(a):
    return jnp.pad(a, ((0, 0), (0, 0), (1, 1), (1, 1), (0, 0)))

def pad_depth(a):
    return jnp.pad(a, ((0, 0), (0, 0), (0, 0), (0, 0), (1, 1)))

def convolve(padded, kernel):
    return lax.conv_general_dilated(pad_depth(padded), kernel, (1, 1, 1), 'VALID', dimension_numbers=('NCDHW', 'OIDHW', 'NCDHW'), preferred_element_type=jnp.float32)

def flipped(kernel):
    return jnp.flip(kernel, (2, 3, 4)).transpose(1, 0, 2, 3, 4)

def correlate(padded, grads):
    wide = pad_depth(padded)
    sx, sy, sz = (grads.shape[2], grads.shape[3], grads.shape[4])
    pieces = []
    for a in range(3):
        for b in range(3):
            for c in range(3):
                window = wide[:, :, a:a + sx, b:b + sy, c:c + sz]
                pieces.append(jnp.einsum('bixyz,boxyz->oi', window, grads, preferred_element_type=jnp.float32))
    stacked = jnp.stack(pieces, axis=0)
    return stacked.reshape(27, grads.shape[1] * padded.shape[1])

def spread(vector):
    return vector[:, :, None, None, None]

def reference(volume, targets, conv1_w, conv1_b, conv2_w, conv2_b, head_w, head_b, dir1, dir2, dir_head):
    high = lax.Precision.HIGHEST
    weight1 = as_kernel(conv1_w, C1, C0)
    weight2 = as_kernel(conv2_w, C2, C1)
    kern1 = as_kernel(dir1.astype(jnp.bfloat16), C1, C0)
    kern2 = as_kernel(dir2.astype(jnp.bfloat16), C2, C1)
    padded_in = pad_plane(volume)
    z1 = convolve(padded_in, weight1) + conv1_b[None, :, None, None, None]
    t1 = convolve(padded_in, kern1)
    act1, slope1, bend1 = silu_parts(z1)
    a1 = act1.astype(jnp.bfloat16)
    ta1 = (slope1 * t1).astype(jnp.bfloat16)
    pa1 = pad_plane(a1)
    pta1 = pad_plane(ta1)
    z2 = convolve(pa1, weight2) + conv2_b[None, :, None, None, None]
    t2 = convolve(pta1, weight2) + convolve(pa1, kern2)
    act2, slope2, bend2 = silu_parts(z2)
    cells = z2.shape[2] * z2.shape[3] * z2.shape[4]
    pooled = lax.optimization_barrier(jnp.sum(act2, axis=(2, 3, 4))) / cells
    tpooled = lax.optimization_barrier(jnp.sum(slope2 * t2, axis=(2, 3, 4))) / cells
    batch = volume.shape[0]
    outputs = jnp.dot(pooled, head_w, precision=high) + head_b
    toutputs = jnp.dot(tpooled, head_w, precision=high) + jnp.dot(pooled, dir_head, precision=high)
    dy = (outputs - targets) / batch
    tdy = toutputs / batch
    hd = jnp.dot(tpooled.T, dy, precision=high) + jnp.dot(pooled.T, tdy, precision=high)
    dpool = jnp.dot(dy, head_w.T, precision=high) / cells
    tdpool = (jnp.dot(tdy, head_w.T, precision=high) + jnp.dot(dy, dir_head.T, precision=high)) / cells
    g2 = (slope2 * spread(dpool)).astype(jnp.bfloat16)
    tg2 = (bend2 * t2 * spread(dpool) + slope2 * spread(tdpool)).astype(jnp.bfloat16)
    h2 = correlate(pa1, tg2) + correlate(pta1, g2)
    pg2 = pad_plane(g2)
    da1 = convolve(pg2, flipped(weight2))
    tda1 = convolve(pad_plane(tg2), flipped(weight2)) + convolve(pg2, flipped(kern2))
    tg1 = (bend1 * t1 * da1 + slope1 * tda1).astype(jnp.bfloat16)
    h1 = correlate(padded_in, tg1)
    field = tda1 * cells
    quad = jnp.sum(dir1 * h1) + jnp.sum(dir2 * h2) + jnp.sum(dir_head * hd)
    length = jnp.sum(dir1 * dir1) + jnp.sum(dir2 * dir2) + jnp.sum(dir_head * dir_head)
    nrm = jnp.sqrt(jnp.sum(h1 * h1) + jnp.sum(h2 * h2) + jnp.sum(hd * hd) + 1e-06)
    return (h1 / nrm, h2 / nrm, hd / nrm, quad / length, field)
```

```python
import jax
import jax.numpy as jnp
from jax import lax
from jax.experimental import pallas as pl
from jax.experimental.pallas import tpu as pltpu
from jax.sharding import PartitionSpec as P

C0 = 4
C1 = 32
C2 = 64
ROWS = 16
REACH = 3
PIECE = 16
Q = 4
VMEM_LIMIT = 24 * 1024 * 1024
F32 = jnp.float32
BF16 = jnp.bfloat16
MESH = pl.DeviceIdType.MESH
NT = (((1,), (1,)), ((), ()))
AXES = ("dp", "gx", "gy")


def silu_parts(z):
    s = 1.0 / (1.0 + jnp.exp(-z))
    return (z * s, s * (1.0 + z * (1.0 - s)), s * (1.0 - s) * (2.0 + z * (1.0 - 2.0 * s)))


def window(ref, cells, taps=range(9)):
    columns = []
    for x, y in cells:
        columns.append(jnp.concatenate([ref[x + tap // 3, y + tap % 3] for tap in taps], axis=0))
    return jnp.concatenate(columns, axis=1)


def iota(shape, dim):
    return lax.broadcasted_iota(jnp.int32, shape, dim)


def channel_pick(rows_inside):
    inside = iota((C2, C2), 0 if rows_inside else 1)
    o = iota((C2, C2), 1 if rows_inside else 0)
    return inside == (o % Q) * (C2 // Q) + o // Q


def column_of(row, pick):
    return jnp.sum(jnp.where(pick, row, 0.0), axis=1, keepdims=True)


def row_of(column, pick):
    return jnp.sum(jnp.where(pick, column, 0.0), axis=0, keepdims=True)


def lanes_from(blocks, width):
    lane = iota(blocks[0].shape, 1)
    out = blocks[-1]
    for j in range(len(blocks) - 2, -1, -1):
        out = jnp.where(lane < (j + 1) * width, blocks[j], out)
    return out


def rolled(u, amount):
    amount %= u.shape[1]
    return pltpu.roll(u, amount, 1) if amount else u


def first_tables():
    wide = 9 * ROWS
    k = iota((32, wide), 0)
    col = iota((32, wide), 1)
    place = (col % ROWS) // C0
    c = jnp.where(place == 0, 1, jnp.where(place == 1, 0, 2))
    spread = jnp.where((place < 3) & (k == 3 * (col // ROWS) + c), 1.0, 0.0).astype(BF16)
    match = (iota((C0 * C1, wide), 0) % C0) == (iota((C0 * C1, wide), 1) % C0)
    fold = jnp.where(iota((C1, C0 * C1), 1) // C0 == iota((C1, C0 * C1), 0), 1.0, 0.0).astype(BF16)
    return spread, match, fold


def lane_of(shape):
    return lax.broadcasted_iota(jnp.int32, shape, len(shape) - 1)


def from_left(u):
    return jnp.where(lane_of(u.shape) == 0, 0.0, pltpu.roll(u, 1, 1))


def from_right(u):
    last = u.shape[1] - 1
    return jnp.where(lane_of(u.shape) == last, 0.0, pltpu.roll(u, last, 1))


def gathered(y, n):
    return from_left(y[:n]) + y[n : 2 * n] + from_right(y[2 * n : 3 * n])


def shifted(ref, cells):
    columns = []
    for x, y in cells:
        u = ref[x, y]
        columns.append(jnp.concatenate([from_right(u), u, from_left(u)], axis=0).astype(BF16))
    return jnp.concatenate(columns, axis=1)


def steps_out(size):
    found = []
    left = REACH
    while left > 0:
        found.append((len(found) + 1, min(size, left)))
        left -= size
    return found


def spans(size):
    found = [(0, 0, REACH, size)]
    for far, count in steps_out(size):
        found.append((far, size - count, REACH - (far - 1) * size - count, count))
        found.append((-far, 0, REACH + far * size, count))
    return found


def pairs_of(cells):
    return [cells[k : k + 2] for k in range(0, len(cells), 2)]


def step_kernel(
    counts, total_cells, batch, stride, per,
    v_hbm, tgt_hbm, w1_hbm, b1_hbm, w2_hbm, b2_hbm, hw_hbm, hb_hbm, k1_hbm, k2_hbm, dh_hbm,
    h_ref, hd_ref, quad_ref, field_ref,
    vin, tgt, w1, b1_in, w2, b2_in, hw_in, hb_in, k1, k2, dh_in,
    vraw, v16, a_ref, ta_ref, d_ref, p_ref, q_ref, g_ref, tg_ref, l2_ref, lb_ref, mb_ref, ms_ref, d2_ref,
    quad_src, quads, pool_src, pools, tgts, hs, rs, ag_src,
    in_sem, v_send, v_recv, pool_send, pool_recv, tgt_send, tgt_recv, rs_send, rs_recv, ag_send, ag_recv, quad_send, quad_recv,
):
    n_dp, n_x, n_y = counts
    n_all = n_dp * n_x * n_y
    _, nx, ny, lanes = vin.shape
    loads = [
        pltpu.make_async_copy(src, dst, in_sem.at[k])
        for k, (src, dst) in enumerate(
            (
                (v_hbm, vin), (w2_hbm, w2), (k2_hbm, k2), (w1_hbm, w1), (k1_hbm, k1), (tgt_hbm, tgt),
                (b1_hbm, b1_in), (b2_hbm, b2_in), (hw_hbm, hw_in), (hb_hbm, hb_in), (dh_hbm, dh_in),
            )
        )
    ]
    for load in loads:
        load.start()

    me_d, me_x, me_y = [lax.axis_index(name) for name in AXES]
    me = (me_d * n_x + me_x) * n_y + me_y

    def coords(flat):
        return (flat // (n_x * n_y), lax.rem(flat // n_y, n_x), lax.rem(flat, n_y))

    def each_other(body):
        if n_all <= 32:
            for r in range(1, n_all):
                body(lax.rem(me + r, n_all))
        else:
            lax.fori_loop(1, n_all, lambda r, c: (body(lax.rem(me + r, n_all)), c)[1], 0)

    barrier = pltpu.get_barrier_semaphore()
    each_other(lambda other: pl.semaphore_signal(barrier, inc=1, device_id=coords(other), device_id_type=MESH))

    def remote(src, dst, send, recv, where):
        return pltpu.make_async_remote_copy(
            src_ref=src, dst_ref=dst, send_sem=send, recv_sem=recv, device_id=where, device_id_type=MESH
        )

    loads[0].wait()
    for x in range(nx):
        planes = [vin[c, x].astype(F32) for c in range(C0)]
        for y in range(ny):
            vraw[REACH + x, REACH + y] = jnp.concatenate([u[y : y + 1] for u in planes], axis=0).astype(BF16)
    for load in loads[1:]:
        load.wait()

    part = C2 // Q
    for kind, ref in enumerate((w2, k2)):
        for c in range(3):
            for g in range(3):
                taps = range(4 * g, min(4 * g + 4, 9))
                rows = [ref[3 * t + c : 3 * t + c + 1, :].astype(F32).reshape(part, Q * C1) for t in taps]
                if kind:
                    for t, u in zip(taps, rows):
                        d2_ref[3 * t + c] = u
                for q in range(Q):
                    block = lanes_from([rolled(u, C1 * (j - q)) for j, u in enumerate(rows)], C1)
                    if len(rows) == 1:
                        block = block[:, :C1]
                    at = (kind * 3 + c) * C2 + q * part
                    l2_ref[at : at + part, 4 * g * C1 : 4 * g * C1 + block.shape[1]] = block.astype(BF16)

    pl.semaphore_wait(barrier, n_all - 1)

    moves = []
    for dx, sx, tx, cx in spans(nx):
        for dy, sy, ty, cy in spans(ny):
            if dx or dy:
                moves.append((dx, dy, sx, tx, cx, sy, ty, cy))

    def inside(dx, dy):
        x, y = me_x + dx, me_y + dy
        return (x >= 0) & (x < n_x) & (y >= 0) & (y < n_y)

    def halo(k):
        dx, dy, sx, tx, cx, sy, ty, cy = moves[k]
        return remote(
            vraw.at[pl.ds(REACH + sx, cx), pl.ds(REACH + sy, cy)], vraw.at[pl.ds(tx, cx), pl.ds(ty, cy)],
            v_send.at[k], v_recv.at[k], (me_d, me_x + dx, me_y + dy),
        )

    for k, (dx, dy, *_) in enumerate(moves):
        @pl.when(inside(dx, dy))
        def _():
            halo(k).start()

    def to_partner(r):
        other = lax.rem(me_d + r, n_dp)
        return remote(tgt, tgts.at[me_d], tgt_send.at[r], tgt_recv.at[r], (other, me_x, me_y))

    for r in range(1, n_dp):
        to_partner(r).start()
    tgts[me_d] = tgt[...]

    for kind in range(2):
        for c in range(3):
            rows = l2_ref[(kind * 3 + c) * C2 : (kind * 3 + c + 1) * C2, :].astype(F32)
            at = (kind * 3 + 2 - c) * C1
            both = jnp.concatenate([rows[:, :128], rows[:, 128:256]], axis=0).T
            for m in range(4):
                lb_ref[at : at + C1, 128 * m : 128 * m + 128] = both[C1 * m : C1 * m + C1].astype(BF16)
            lb_ref[at : at + C1, 512:] = rows[:, 256:].T.astype(BF16)
    back = [8 - t for t in (0, 4, 1, 5, 2, 6, 3, 7, 8)]

    spread, match, fold = first_tables()
    l1 = []
    high = k1[...].astype(BF16)
    for flat in (w1[...], high, (k1[...] - high.astype(F32)).astype(BF16)):
        flat = jnp.concatenate([flat.astype(F32), jnp.zeros((5, C0 * C1), F32)], axis=0)
        wide = jnp.dot(flat.T.astype(BF16), spread, preferred_element_type=F32)
        wide = jnp.where(match, wide, 0.0).astype(BF16)
        l1.append(jnp.dot(fold, wide, preferred_element_type=F32))
    d1 = l1[1] + l1[2]
    l1 = jnp.concatenate(l1[:2], axis=0).astype(BF16)
    b1 = column_of(b1_in[...], iota((C1, C1), 0) == iota((C1, C1), 1))
    inside_rows = channel_pick(True)
    outside_rows = channel_pick(False)
    b2 = column_of(b2_in[...], inside_rows)
    outs = hw_in.shape[0]
    square = iota((C2, C2), 0) == iota((C2, C2), 1)

    def moved_rows(whole, pick):
        return jnp.concatenate(
            [row_of(column_of(whole[m : m + 1], pick), square) for m in range(outs)], axis=0
        )

    def head_rows(ref):
        return moved_rows(ref[...], inside_rows)

    hw, dh = head_rows(hw_in), head_rows(dh_in)
    small = iota((outs, outs), 0) == iota((outs, outs), 1)
    hb = column_of(hb_in[...], small)

    def arrive(near):
        for k, (dx, dy, sx, tx, cx, sy, ty, cy) in enumerate(moves):
            if (abs(dx) <= 1 and abs(dy) <= 1) == near:
                came = inside(-dx, -dy)

                @pl.when(came)
                def _():
                    halo(k).wait_recv()

                @pl.when(jnp.logical_not(came))
                def _():
                    vraw[tx : tx + cx, ty : ty + cy] = jnp.zeros((cx, cy, C0, lanes), BF16)

    sub = iota((8, lanes), 0)

    def expand(cells):
        for x, y in cells:
            u = vraw[x, y].astype(F32)
            full = jnp.concatenate([u, u], axis=0)
            top = jnp.where(sub < C0, full, from_left(full))
            low = jnp.where(sub < C0, from_right(full), 0.0)
            v16[x, y] = jnp.concatenate([top, low], axis=0).astype(BF16)

    def valid(x, y):
        gx, gy = me_x * nx + x, me_y * ny + y
        return jnp.where((gx >= 0) & (gx < n_x * nx) & (gy >= 0) & (gy < n_y * ny), 1.0, 0.0).astype(F32)

    def first_block(cells):
        for pair in pairs_of(cells):
            res = jnp.dot(l1, window(v16, pair), preferred_element_type=F32)
            for k, (x, y) in enumerate(pair):
                part = res[:, k * lanes : (k + 1) * lanes]
                t1 = part[C1:]
                act, slope, bend = silu_parts(part[:C1] + b1)
                mine = 2 <= x < nx + 2 and 2 <= y < ny + 2
                if mine:
                    a_ref[x, y] = act.astype(BF16)
                    ta_ref[x, y] = (slope * t1).astype(BF16)
                    d_ref[0, x - 2, y - 2] = slope
                    d_ref[1, x - 2, y - 2] = bend * t1
                else:
                    mask = valid(x - 2, y - 2)
                    a_ref[x, y] = (act * mask).astype(BF16)
                    ta_ref[x, y] = (slope * t1 * mask).astype(BF16)

    n2 = 3 * C2

    def second_block(cells, sums):
        for pair in pairs_of(cells):
            res = jnp.dot(l2_ref[...], window(a_ref, pair), preferred_element_type=F32)
            tres = res[n2:] + jnp.dot(l2_ref[:n2], window(ta_ref, pair), preferred_element_type=F32)
            for k, (x, y) in enumerate(pair):
                z2 = gathered(res[:n2, k * lanes : (k + 1) * lanes], C2) + b2
                t2 = gathered(tres[:, k * lanes : (k + 1) * lanes], C2)
                act, slope, bend = silu_parts(z2)
                if sums is not None:
                    sums = (sums[0] + act, sums[1] + slope * t2)
                    p_ref[x, y] = slope
                    q_ref[x, y] = bend * t2
                else:
                    mask = valid(x - 1, y - 1)
                    p_ref[x, y] = slope * mask
                    q_ref[x, y] = bend * t2 * mask
        return sums

    def box(x0, x1, y0, y1):
        return [(x, y) for x in range(x0, x1) for y in range(y0, y1)]

    near_v = box(1, nx + 5, 1, ny + 5)
    far_v = [c for c in box(0, nx + 6, 0, ny + 6) if c not in near_v]
    near_a = box(1, nx + 3, 1, ny + 3)
    far_a = [c for c in box(0, nx + 4, 0, ny + 4) if c not in near_a]
    own_z = box(1, nx + 1, 1, ny + 1)
    far_z = [c for c in box(0, nx + 2, 0, ny + 2) if c not in own_z]

    arrive(True)
    expand(near_v)
    first_block(near_a)
    zero = jnp.zeros((C2, lanes), F32)
    sums = second_block(own_z, (zero, zero))
    row = jnp.sum(jnp.concatenate(sums, axis=0).T, axis=0, keepdims=True)
    pool_src[...] = row

    def pool_to(other):
        return remote(pool_src, pools.at[me], pool_send, pool_recv, coords(other))

    each_other(lambda other: pool_to(other).start())
    pools[me] = row

    arrive(False)
    expand(far_v)
    first_block(far_a)
    second_block(far_z, None)

    cut = 8 * C1
    m_most = jnp.zeros((2 * n2, cut), F32)
    m_rest = jnp.zeros((C1, 2 * n2), F32)
    n_most = jnp.zeros((n2, cut), F32)
    n_rest = jnp.zeros((C1, n2), F32)
    for pair in pairs_of(own_z):
        gs = shifted(p_ref, pair)
        both = jnp.concatenate([shifted(q_ref, pair), gs], axis=0)
        u = window(a_ref, pair)
        m_most = m_most + lax.dot_general(both, u[:cut], NT, preferred_element_type=F32)
        m_rest = m_rest + lax.dot_general(u[cut:], both, NT, preferred_element_type=F32)
        u = window(ta_ref, pair)
        n_most = n_most + lax.dot_general(gs, u[:cut], NT, preferred_element_type=F32)
        n_rest = n_rest + lax.dot_general(u[cut:], gs, NT, preferred_element_type=F32)
    for ref, most, rest in (
        (mb_ref, m_most[:n2] + n_most, m_rest[:, :n2] + n_rest),
        (ms_ref, m_most[n2:], m_rest[:, n2:]),
    ):
        rest = rest.T
        for c in range(3):
            rows = [most[c * C2 + q * part : c * C2 + (q + 1) * part] for q in range(Q)]
            for t in range(8):
                cols = slice(128 * (t // 4), 128 * (t // 4) + 128)
                ref[3 * t + c] = lanes_from([rolled(u[:, cols], C1 * (q - t % 4)) for q, u in enumerate(rows)], C1)
            rows = [rest[c * C2 + q * part : c * C2 + (q + 1) * part] for q in range(Q)]
            ref[24 + c] = jnp.concatenate(rows, axis=1)

    def wait_many(buf, count, sem):
        part = buf.at[pl.ds(0, count)]
        pltpu.make_async_copy(part, part, sem).wait()

    wait_many(pools, n_all - 1, pool_recv)
    for r in range(1, n_dp):
        to_partner(r).wait_recv()

    hd = jnp.zeros((outs, C2), F32)
    dpool = jnp.zeros((1, C2), F32)
    tdpool = jnp.zeros((1, C2), F32)
    group = n_x * n_y
    for d in range(n_dp):
        pair = jnp.sum(pools[d * group : (d + 1) * group], axis=0) / total_cells
        pooled, tpooled = pair[:, :C2], pair[:, C2:]
        out = jnp.sum(hw * pooled, axis=1, keepdims=True) + hb
        tout = jnp.sum(hw * tpooled + dh * pooled, axis=1, keepdims=True)
        dy = (out - column_of(tgts[d], small)) / batch
        tdy = tout / batch
        hd = hd + (tpooled * dy + pooled * tdy)
        dp = jnp.sum(dy * hw, axis=0, keepdims=True) / total_cells
        tdp = jnp.sum(tdy * hw + dy * dh, axis=0, keepdims=True) / total_cells
        dpool = jnp.where(me_d == d, dp, dpool)
        tdpool = jnp.where(me_d == d, tdp, tdpool)

    dcol, tcol = column_of(dpool, square), column_of(tdpool, square)

    def tile_of(column):
        return lanes_from(
            [jnp.broadcast_to(column[q * part : (q + 1) * part], (part, Q * C1)) for q in range(Q)], C1
        )

    dtile, ttile = tile_of(dcol), tile_of(tcol)
    owners = hs.shape[0]
    early = 27 // per

    def part_to(j):
        return remote(hs.at[j], rs.at[me], rs_send, rs_recv, coords(j * stride))

    def put(piece, block):
        at = piece % per * PIECE
        hs[piece // per, at : at + PIECE] = block.astype(BF16)

    def send_parts(first, last):
        for j in range(first, last):
            @pl.when(me != j * stride)
            def _():
                part_to(j).start()

    quad = jnp.zeros((PIECE, 128), F32)
    for k in range(27):
        term = mb_ref[k] * dtile + ms_ref[k] * ttile
        put(k, term)
        quad = quad + term * d2_ref[k]
    send_parts(0, early)

    for x, y in box(0, nx + 2, 0, ny + 2):
        slope = p_ref[x, y]
        g_ref[x, y] = (slope * dcol).astype(BF16)
        tg_ref[x, y] = (q_ref[x, y] * dcol + slope * tcol).astype(BF16)

    n1 = 3 * C1
    h1 = jnp.zeros((C1, 9 * ROWS), F32)
    for pair in pairs_of(box(0, nx, 0, ny)):
        res = jnp.dot(lb_ref[...], window(g_ref, pair, back), preferred_element_type=F32)
        tres = res[n1:] + jnp.dot(lb_ref[:n1], window(tg_ref, pair, back), preferred_element_type=F32)
        grads = []
        for k, (x, y) in enumerate(pair):
            da = gathered(res[:n1, k * lanes : (k + 1) * lanes], C1)
            tda = gathered(tres[:, k * lanes : (k + 1) * lanes], C1)
            field_ref[:, x, y, :] = tda * total_cells
            grads.append((d_ref[1, x, y] * da + d_ref[0, x, y] * tda).astype(BF16))
        around = [(x + 2, y + 2) for x, y in pair]
        h1 = h1 + lax.dot_general(
            jnp.concatenate(grads, axis=1), window(v16, around), NT, preferred_element_type=F32
        )
    own1 = jnp.sum(d1 * h1, axis=0, keepdims=True)
    tail1 = jnp.concatenate([own1[:, 128:], jnp.zeros((1, 256 - 9 * ROWS), F32)], axis=1)
    quad = jnp.sum(quad, axis=0, keepdims=True) + own1[:, :128] + tail1
    quad_src[...] = quad
    wide = lax.dot_general(fold, h1.astype(BF16), (((0,), (0,)), ((), ())), preferred_element_type=F32)
    wide = jnp.where(match, wide, 0.0).astype(BF16)
    flat = lax.dot_general(spread, wide, NT, preferred_element_type=F32)
    for k in range(27, owners * per):
        put(k, flat[(k - 27) * PIECE : (k - 26) * PIECE] if k < 29 else jnp.zeros((PIECE, 128), F32))
    send_parts(early, owners)

    def quad_to(other):
        return remote(quad_src, quads.at[me], quad_send, quad_recv, coords(other))

    each_other(lambda other: quad_to(other).start())
    quads[me] = quad

    hd_ref[...] = moved_rows(hd, outside_rows)

    def head_row(u):
        return jnp.concatenate([jnp.sum(u, axis=0, keepdims=True), jnp.zeros((1, 128 - C2), F32)], axis=1)


    slot = me // stride
    is_owner = lax.rem(me, stride) == 0
    if owners * stride != n_all:
        is_owner = is_owner & (slot < owners)

    def total_to(other):
        return remote(ag_src, h_ref.at[slot], ag_send, ag_recv, coords(other))

    def own():
        wait_many(rs, n_all - 1, rs_recv)
        rs[me] = hs[slot]
        terms = [rs[k].astype(F32) for k in range(n_all)]
        while len(terms) > 1:
            terms = [sum(terms[k : k + 2]) for k in range(0, len(terms), 2)]
        mine = terms[0].astype(BF16)
        ag_src[...] = mine
        each_other(lambda other: total_to(other).start())
        h_ref[slot] = mine
        wait_many(h_ref, owners - 1, ag_recv)
        wait_many(hs, owners - 1, rs_send)
        wait_many(rs, n_all - 1, ag_send)

    def rest_of():
        wait_many(h_ref, owners, ag_recv)
        wait_many(hs, owners, rs_send)

    if owners == n_all:
        own()
    else:
        pl.when(is_owner)(own)
        pl.when(jnp.logical_not(is_owner))(rest_of)

    for k, (dx, dy, *_) in enumerate(moves):
        @pl.when(inside(dx, dy))
        def _():
            halo(k).wait_send()

    for r in range(1, n_dp):
        to_partner(r).wait_send()
    wait_many(pools, n_all - 1, pool_send)
    wait_many(quads, n_all - 1, quad_recv)
    wait_many(quads, n_all - 1, quad_send)
    quad_ref[0:1, :] = jnp.sum(quads[...], axis=0) + head_row(dh * hd)
    quad_ref[1:2, :] = head_row(dh * dh)


def last_kernel(
    per, h_ref, hd_ref, quad_ref, field_in, dir1_ref, dir2_ref,
    next1_ref, next2_ref, head_ref, ray_ref, field_out, sem,
):
    copy = pltpu.make_async_copy(field_in, field_out, sem)
    copy.start()
    h = h_ref[...].astype(F32).reshape(-1, 128)
    h1 = h[27 * PIECE : 27 * PIECE + 27]
    hd = hd_ref[...]
    dir1 = dir1_ref[...]
    rows = [h[k * PIECE : (k + 1) * PIECE].reshape(1, PIECE * 128) for k in range(27)]
    h2 = jnp.concatenate(rows, axis=0)
    dir2 = dir2_ref[...]

    def total(u):
        u = jnp.sum(u, axis=0, keepdims=True)
        return u if u.shape[1] == 128 else sum(u[:, j : j + 128] for j in range(0, u.shape[1], 128))

    def across(u):
        return jnp.sum(u, axis=1, keepdims=True)

    quad = across(quad_ref[0:1, :])
    length = across(total(dir1 * dir1) + total(dir2 * dir2) + quad_ref[1:2, :])
    head = jnp.sum(hd * hd, axis=0, keepdims=True)
    nrm = jnp.sqrt(across(total(h1 * h1) + total(h2 * h2)) + across(head) + 1e-06)
    scale = 1.0 / nrm
    next1_ref[...] = h1 * scale
    next2_ref[...] = h2 * scale
    head_ref[...] = hd * scale
    ray_ref[...] = quad / length
    copy.wait()


def per_device(
    volume, targets, conv1_w, conv1_b, conv2_w, conv2_b, head_w, head_b, dir1, dir2, dir_head
):
    nx, ny, lanes = volume.shape[2:]
    counts = tuple(lax.axis_size(name) for name in AXES)
    n_all = counts[0] * counts[1] * counts[2]
    total_cells = nx * counts[1] * ny * counts[2] * lanes
    batch = volume.shape[0] * counts[0]
    outs = head_w.shape[1]
    per = max(1, -(-29 // n_all))
    owners = -(-29 // per)
    stride = n_all // owners
    n_moves = len(spans(nx)) * len(spans(ny)) - 1
    shape = jax.ShapeDtypeStruct
    dma = pltpu.SemaphoreType.DMA
    hbm = pl.BlockSpec(memory_space=pltpu.HBM)
    args = (
        volume[0], targets, conv1_w, conv1_b[None], conv2_w, conv2_b[None], head_w.T, head_b[None], dir1, dir2, dir_head.T
    )

    args = tuple(pltpu.with_memory_space_constraint(a, pltpu.HBM) for a in args)

    def kernel(*refs):
        step_kernel(counts, total_cells, batch, stride, per, *refs)

    h, hd, quad, field = pl.pallas_call(
        kernel,
        in_specs=[hbm] * len(args),
        out_shape=(
            shape((owners, per * PIECE, 128), BF16),
            shape((outs, C2), F32),
            shape((2, 128), F32),
            shape((C1, nx, ny, lanes), F32),
        ),
        scratch_shapes=[pltpu.VMEM(a.shape, a.dtype) for a in args]
        + [
            pltpu.VMEM((nx + 6, ny + 6, C0, lanes), BF16),
            pltpu.VMEM((nx + 6, ny + 6, ROWS, lanes), BF16),
            pltpu.VMEM((nx + 4, ny + 4, C1, lanes), BF16),
            pltpu.VMEM((nx + 4, ny + 4, C1, lanes), BF16),
            pltpu.VMEM((2, nx, ny, C1, lanes), F32),
            pltpu.VMEM((nx + 2, ny + 2, C2, lanes), F32),
            pltpu.VMEM((nx + 2, ny + 2, C2, lanes), F32),
            pltpu.VMEM((nx + 2, ny + 2, C2, lanes), BF16),
            pltpu.VMEM((nx + 2, ny + 2, C2, lanes), BF16),
            pltpu.VMEM((6 * C2, 9 * C1), BF16),
            pltpu.VMEM((6 * C1, 9 * C2), BF16),
            pltpu.VMEM((27, PIECE, 128), F32),
            pltpu.VMEM((27, PIECE, 128), F32),
            pltpu.VMEM((27, PIECE, 128), F32),
            pltpu.VMEM((1, 128), F32),
            pltpu.VMEM((n_all, 1, 128), F32),
            pltpu.VMEM((1, 2 * C2), F32),
            pltpu.VMEM((n_all, 1, 2 * C2), F32),
            pltpu.VMEM((counts[0], 1, outs), F32),
            pltpu.VMEM((owners, per * PIECE, 128), BF16),
            pltpu.VMEM((n_all, per * PIECE, 128), BF16),
            pltpu.VMEM((per * PIECE, 128), BF16),
            dma((len(args),)), dma((n_moves,)), dma((n_moves,)), dma, dma, dma((counts[0],)), dma((counts[0],)),
            dma, dma, dma, dma, dma, dma,
        ],
        compiler_params=pltpu.CompilerParams(
            collective_id=0, has_side_effects=True, vmem_limit_bytes=VMEM_LIMIT
        ),
    )(*args)

    def last(*refs):
        last_kernel(per, *refs)

    vmem = pl.BlockSpec(memory_space=pltpu.VMEM)
    next1, next2, head, ray, field = pl.pallas_call(
        last,
        in_specs=[vmem] * 6,
        out_specs=(vmem, vmem, vmem, vmem, hbm),
        out_shape=(
            shape(dir1.shape, F32), shape(dir2.shape, F32), shape((outs, C2), F32), shape((1, 1), F32),
            shape(field.shape, F32),
        ),
        scratch_shapes=[dma],
        compiler_params=pltpu.CompilerParams(vmem_limit_bytes=VMEM_LIMIT),
    )(h, hd, quad, field, dir1, dir2)
    return (next1, next2, head.T, ray[0, 0], field[None])


def solution(mesh):
    return jax.shard_map(
        per_device,
        mesh=mesh,
        in_specs=(P("dp", None, "gx", "gy", None), P("dp", None)) + (P(),) * 9,
        out_specs=(P(), P(), P(), P(), P("dp", None, "gx", "gy", None)),
        check_vma=False,
    )
```

```python
import jax
import jax.numpy as jnp
from jax import lax
from jax.experimental import pallas as pl
from jax.experimental.pallas import tpu as pltpu
from jax.sharding import PartitionSpec as P

C0 = 4
C1 = 32
C2 = 64
ROWS = 16
REACH = 3
PIECE = 16
Q = 4
VMEM_LIMIT = 24 * 1024 * 1024
F32 = jnp.float32
BF16 = jnp.bfloat16
MESH = pl.DeviceIdType.MESH
NT = (((1,), (1,)), ((), ()))
AXES = ("dp", "gx", "gy")


def silu_parts(z):
    s = 0.5 * jnp.tanh(0.5 * z) + 0.5
    act = z * s
    u = 1.0 - s
    return (act, s + act * u, s * u * ((2.0 + z) - (act + act)))


def window(ref, cells, taps=range(9)):
    columns = []
    for x, y in cells:
        columns.append(jnp.concatenate([ref[x + tap // 3, y + tap % 3] for tap in taps], axis=0))
    return jnp.concatenate(columns, axis=1)


def iota(shape, dim):
    return lax.broadcasted_iota(jnp.int32, shape, dim)


def channel_pick(rows_inside):
    inside = iota((C2, C2), 0 if rows_inside else 1)
    o = iota((C2, C2), 1 if rows_inside else 0)
    return inside == (o % Q) * (C2 // Q) + o // Q


def column_of(row, pick):
    return jnp.sum(jnp.where(pick, row, 0.0), axis=1, keepdims=True)


def row_of(column, pick):
    return jnp.sum(jnp.where(pick, column, 0.0), axis=0, keepdims=True)


def lanes_from(blocks, width):
    lane = iota(blocks[0].shape, 1)
    out = blocks[-1]
    for j in range(len(blocks) - 2, -1, -1):
        out = jnp.where(lane < (j + 1) * width, blocks[j], out)
    return out


def rolled(u, amount):
    amount %= u.shape[1]
    return pltpu.roll(u, amount, 1) if amount else u


def first_tables():
    wide = 9 * ROWS
    k = iota((32, wide), 0)
    col = iota((32, wide), 1)
    place = (col % ROWS) // C0
    c = jnp.where(place == 0, 1, jnp.where(place == 1, 0, 2))
    spread = jnp.where((place < 3) & (k == 3 * (col // ROWS) + c), 1.0, 0.0).astype(BF16)
    match = (iota((C0 * C1, wide), 0) % C0) == (iota((C0 * C1, wide), 1) % C0)
    fold = jnp.where(iota((C1, C0 * C1), 1) // C0 == iota((C1, C0 * C1), 0), 1.0, 0.0).astype(BF16)
    return spread, match, fold


def lane_of(shape):
    return lax.broadcasted_iota(jnp.int32, shape, len(shape) - 1)


def from_left(u):
    return jnp.where(lane_of(u.shape) == 0, 0.0, pltpu.roll(u, 1, 1))


def from_right(u):
    last = u.shape[1] - 1
    return jnp.where(lane_of(u.shape) == last, 0.0, pltpu.roll(u, last, 1))


def gathered(y, n):
    return from_left(y[:n]) + y[n : 2 * n] + from_right(y[2 * n : 3 * n])


def shifted(ref, cells):
    columns = []
    for x, y in cells:
        u = ref[x, y]
        columns.append(jnp.concatenate([from_right(u), u, from_left(u)], axis=0).astype(BF16))
    return jnp.concatenate(columns, axis=1)


def steps_out(size):
    found = []
    left = REACH
    while left > 0:
        found.append((len(found) + 1, min(size, left)))
        left -= size
    return found


def spans(size):
    found = [(0, 0, REACH, size)]
    for far, count in steps_out(size):
        found.append((far, size - count, REACH - (far - 1) * size - count, count))
        found.append((-far, 0, REACH + far * size, count))
    return found


def pairs_of(cells):
    return [cells[k : k + 2] for k in range(0, len(cells), 2)]


def step_kernel(
    counts, total_cells, batch, stride, per,
    v_hbm, tgt_hbm, w1_hbm, b1_hbm, w2_hbm, b2_hbm, hw_hbm, hb_hbm, k1_hbm, k2_hbm, dh_hbm,
    h_ref, hd_ref, quad_ref, field_ref,
    vin, tgt, w1, b1_in, w2, b2_in, hw_in, hb_in, k1, k2, dh_in,
    vraw, v16, a_ref, ta_ref, d_ref, p_ref, q_ref, g_ref, tg_ref, l2_ref, lb_ref, l2r_ref, lbr_ref, mb_ref, ms_ref, d2_ref,
    quad_src, quads, pool_src, pools, tgts, hs, rs, ag_src,
    in_sem, v_send, v_recv, pool_send, pool_recv, tgt_send, tgt_recv, rs_send, rs_recv, ag_send, ag_recv, quad_send, quad_recv, round_sem,
):
    n_dp, n_x, n_y = counts
    n_all = n_dp * n_x * n_y
    _, nx, ny, lanes = vin.shape
    loads = [
        pltpu.make_async_copy(src, dst, in_sem.at[k])
        for k, (src, dst) in enumerate(
            (
                (v_hbm, vin), (w2_hbm, w2), (k2_hbm, k2), (w1_hbm, w1), (k1_hbm, k1), (tgt_hbm, tgt),
                (b1_hbm, b1_in), (b2_hbm, b2_in), (hw_hbm, hw_in), (hb_hbm, hb_in), (dh_hbm, dh_in),
            )
        )
    ]
    me_d, me_x, me_y = [lax.axis_index(name) for name in AXES]
    me = (me_d * n_x + me_x) * n_y + me_y

    def coords(flat):
        return (flat // (n_x * n_y), lax.rem(flat // n_y, n_x), lax.rem(flat, n_y))

    def ring(at, count):
        after = [at]
        for k in range(1, count):
            after.append(jnp.where(at + k >= count, at + k - count, at + k))
        return after[1:] + after[:1]

    rings = ring(me_d, n_dp), ring(me_x, n_x), ring(me_y, n_y)

    def each_other(body):
        if n_all <= 32:
            everyone = [(d, x, y) for y in rings[2] for x in rings[1] for d in rings[0]]
            for where in everyone[:-1]:
                body(where)
        else:
            lax.fori_loop(1, n_all, lambda r, c: (body(coords(lax.rem(me + r, n_all))), c)[1], 0)

    barrier = pltpu.get_barrier_semaphore()
    reach_x, reach_y = len(steps_out(nx)), len(steps_out(ny))
    rounds = round_sem.shape[0]

    def inside(dx, dy):
        x, y = me_x + dx, me_y + dy
        return (x >= 0) & (x < n_x) & (y >= 0) & (y < n_y)

    def held(at, count, reach):
        return jnp.minimum(at, reach) + jnp.minimum(count - 1 - at, reach) + 1

    def tell(sem, far_x, far_y, cores):
        for dx in range(-far_x, far_x + 1):
            for dy in range(-far_y, far_y + 1):
                if dx or dy:
                    @pl.when(inside(dx, dy))
                    def _():
                        for d in cores:
                            pl.semaphore_signal(
                                sem, inc=1, device_id=(d, me_x + dx, me_y + dy), device_id_type=MESH
                            )
        for d in cores[:-1]:
            pl.semaphore_signal(sem, inc=1, device_id=(d, me_x, me_y), device_id_type=MESH)

    def tell_round(k):
        tell(round_sem.at[k], 1, 1, [me_d])

    def hear_round(k):
        pl.semaphore_wait(round_sem.at[k], held(me_x, n_x, 1) * held(me_y, n_y, 1) - 1)

    tell(barrier, reach_x, reach_y, rings[0])

    def remote(src, dst, send, recv, where):
        return pltpu.make_async_remote_copy(
            src_ref=src, dst_ref=dst, send_sem=send, recv_sem=recv, device_id=where, device_id_type=MESH
        )

    for load in loads:
        load.start()
    loads[0].wait()
    for x in range(nx):
        planes = [vin[c, x].astype(F32) for c in range(C0)]
        for y in range(ny):
            vraw[REACH + x, REACH + y] = jnp.concatenate([u[y : y + 1] for u in planes], axis=0).astype(BF16)
    for load in loads[1:]:
        load.wait()

    part = C2 // Q
    lane = iota((part, Q * C1), 1)
    for kind, ref in enumerate((w2, k2)):
        for c in range(3):
            for g in range(3):
                taps = range(4 * g, min(4 * g + 4, 9))
                rows = [ref[3 * t + c : 3 * t + c + 1, :].astype(F32).reshape(part, Q * C1) for t in taps]
                if kind:
                    for t, u in zip(taps, rows):
                        d2_ref[3 * t + c] = u
                for q in range(Q):
                    block = lanes_from([rolled(u, C1 * (j - q)) for j, u in enumerate(rows)], C1)
                    at = (kind * 3 + c) * C2 + q * part
                    if len(rows) == 1:
                        if kind == 0:
                            beside = rolled(rows[0], C1 - C1 * q)
                            l2r_ref[at : at + part] = jnp.where(lane < C1, block, 0.0)[:, : 2 * C1].astype(BF16)
                            l2r_ref[at + 3 * C2 : at + 3 * C2 + part] = beside[:, : 2 * C1].astype(BF16)
                        block = block[:, :C1]
                        if kind == 1:
                            l2r_ref[at : at + part, :C1] = block.astype(BF16)
                    l2_ref[at : at + part, 4 * g * C1 : 4 * g * C1 + block.shape[1]] = block.astype(BF16)

    pl.semaphore_wait(barrier, n_dp * held(me_x, n_x, reach_x) * held(me_y, n_y, reach_y) - 1)

    moves = []
    for dx, sx, tx, cx in spans(nx):
        for dy, sy, ty, cy in spans(ny):
            if dx or dy:
                moves.append((dx, dy, sx, tx, cx, sy, ty, cy))

    def halo(k):
        dx, dy, sx, tx, cx, sy, ty, cy = moves[k]
        return remote(
            vraw.at[pl.ds(REACH + sx, cx), pl.ds(REACH + sy, cy)], vraw.at[pl.ds(tx, cx), pl.ds(ty, cy)],
            v_send.at[k], v_recv.at[k], (me_d, me_x + dx, me_y + dy),
        )

    for k, (dx, dy, *_) in enumerate(moves):
        @pl.when(inside(dx, dy))
        def _():
            halo(k).start()

    def to_partner(r):
        other = lax.rem(me_d + r, n_dp)
        return remote(tgt, tgts.at[me_d], tgt_send.at[r], tgt_recv.at[r], (other, me_x, me_y))

    for r in range(1, n_dp):
        to_partner(r).start()
    tgts[me_d] = tgt[...]
    tell_round(0)

    for kind in range(2):
        for c in range(3):
            rows = l2_ref[(kind * 3 + c) * C2 : (kind * 3 + c + 1) * C2, :].astype(F32)
            at = (kind * 3 + 2 - c) * C1
            both = jnp.concatenate([rows[:, :128], rows[:, 128:256]], axis=0).T
            for m in range(4):
                lb_ref[at : at + C1, 128 * m : 128 * m + 128] = both[C1 * m : C1 * m + C1].astype(BF16)
            end = rows[:, 256:].T.astype(BF16)
            none = jnp.zeros((C1, C2), BF16)
            if kind == 0:
                lbr_ref[at : at + C1] = jnp.concatenate([end, none], axis=1)
                lbr_ref[at + 3 * C1 : at + 4 * C1] = jnp.concatenate([none, end], axis=1)
            else:
                lbr_ref[at : at + C1, :C2] = end
    back = [8 - t for t in (0, 4, 1, 5, 2, 6, 3, 7, 8)]

    spread, match, fold = first_tables()
    l1 = []
    high = k1[...].astype(BF16)
    for flat in (w1[...], high, (k1[...] - high.astype(F32)).astype(BF16)):
        flat = jnp.concatenate([flat.astype(F32), jnp.zeros((5, C0 * C1), F32)], axis=0)
        wide = jnp.dot(flat.T.astype(BF16), spread, preferred_element_type=F32)
        wide = jnp.where(match, wide, 0.0).astype(BF16)
        l1.append(jnp.dot(fold, wide, preferred_element_type=F32))
    d1 = l1[1] + l1[2]
    l1 = jnp.concatenate(l1[:2], axis=0).astype(BF16)
    b1 = column_of(b1_in[...], iota((C1, C1), 0) == iota((C1, C1), 1))
    inside_rows = channel_pick(True)
    outside_rows = channel_pick(False)
    b2 = column_of(b2_in[...], inside_rows)
    outs = hw_in.shape[0]
    square = iota((C2, C2), 0) == iota((C2, C2), 1)

    def moved_rows(whole, pick):
        return jnp.concatenate(
            [row_of(column_of(whole[m : m + 1], pick), square) for m in range(outs)], axis=0
        )

    def head_rows(ref):
        return moved_rows(ref[...], inside_rows)

    hw, dh = head_rows(hw_in), head_rows(dh_in)
    small = iota((outs, outs), 0) == iota((outs, outs), 1)
    hb = column_of(hb_in[...], small)

    def arrive(near):
        for k, (dx, dy, sx, tx, cx, sy, ty, cy) in enumerate(moves):
            if (abs(dx) <= 1 and abs(dy) <= 1) == near:
                came = inside(-dx, -dy)

                @pl.when(came)
                def _():
                    halo(k).wait_recv()

                @pl.when(jnp.logical_not(came))
                def _():
                    vraw[tx : tx + cx, ty : ty + cy] = jnp.zeros((cx, cy, C0, lanes), BF16)

    sub = iota((8, lanes), 0)

    def expand(cells):
        for x, y in cells:
            u = vraw[x, y].astype(F32)
            full = jnp.concatenate([u, u], axis=0)
            top = jnp.where(sub < C0, full, from_left(full))
            low = jnp.where(sub < C0, from_right(full), 0.0)
            v16[x, y] = jnp.concatenate([top, low], axis=0).astype(BF16)

    def valid(x, y):
        gx, gy = me_x * nx + x, me_y * ny + y
        return jnp.where((gx >= 0) & (gx < n_x * nx) & (gy >= 0) & (gy < n_y * ny), 1.0, 0.0).astype(F32)

    def first_block(cells):
        for pair in pairs_of(cells):
            res = jnp.dot(l1, window(v16, pair), preferred_element_type=F32)
            for k, (x, y) in enumerate(pair):
                part = res[:, k * lanes : (k + 1) * lanes]
                t1 = part[C1:]
                act, slope, bend = silu_parts(part[:C1] + b1)
                mine = 2 <= x < nx + 2 and 2 <= y < ny + 2
                if mine:
                    a_ref[x, y] = act.astype(BF16)
                    ta_ref[x, y] = (slope * t1).astype(BF16)
                    d_ref[0, x - 2, y - 2] = slope
                    d_ref[1, x - 2, y - 2] = bend * t1
                else:
                    mask = valid(x - 2, y - 2)
                    a_ref[x, y] = (act * mask).astype(BF16)
                    ta_ref[x, y] = (slope * t1 * mask).astype(BF16)

    n2 = 3 * C2

    def second_block(cells, sums):
        for pair in pairs_of(cells):
            end = jnp.concatenate([window(a_ref, pair, (8,)), window(ta_ref, pair, (8,))], axis=0)
            res = jnp.dot(l2_ref[:, : 8 * C1], window(a_ref, pair, range(8)), preferred_element_type=F32)
            res = res + jnp.dot(l2r_ref[...], end, preferred_element_type=F32)
            tres = jnp.dot(l2_ref[:n2, : 8 * C1], window(ta_ref, pair, range(8)), preferred_element_type=F32)
            tres = res[n2:] + tres
            for k, (x, y) in enumerate(pair):
                z2 = gathered(res[:n2, k * lanes : (k + 1) * lanes], C2) + b2
                t2 = gathered(tres[:, k * lanes : (k + 1) * lanes], C2)
                act, slope, bend = silu_parts(z2)
                if sums is not None:
                    sums = (sums[0] + act, sums[1] + slope * t2)
                    p_ref[x, y] = slope
                    q_ref[x, y] = bend * t2
                else:
                    mask = valid(x - 1, y - 1)
                    p_ref[x, y] = slope * mask
                    q_ref[x, y] = bend * t2 * mask
        return sums

    def box(x0, x1, y0, y1):
        return [(x, y) for x in range(x0, x1) for y in range(y0, y1)]

    near_v = box(1, nx + 5, 1, ny + 5)
    far_v = [c for c in box(0, nx + 6, 0, ny + 6) if c not in near_v]
    near_a = box(1, nx + 3, 1, ny + 3)
    far_a = [c for c in box(0, nx + 4, 0, ny + 4) if c not in near_a]
    own_z = box(1, nx + 1, 1, ny + 1)
    far_z = [c for c in box(0, nx + 2, 0, ny + 2) if c not in own_z]

    for k in range(rounds - 1):
        hear_round(k)
        tell_round(k + 1)
    arrive(True)
    expand(near_v)
    first_block(near_a)
    zero = jnp.zeros((C2, lanes), F32)
    sums = second_block(own_z, (zero, zero))
    row = jnp.sum(jnp.concatenate(sums, axis=0).T, axis=0, keepdims=True)
    pool_src[...] = row

    def pool_to(where):
        return remote(pool_src, pools.at[me], pool_send, pool_recv, where)

    hear_round(rounds - 1)
    each_other(lambda where: pool_to(where).start())
    pools[me] = row

    arrive(False)
    expand(far_v)
    first_block(far_a)
    second_block(far_z, None)

    cut = 8 * C1
    m_most = jnp.zeros((2 * n2, cut), F32)
    m_rest = jnp.zeros((C1, 2 * n2), F32)
    n_most = jnp.zeros((n2, cut), F32)
    n_rest = jnp.zeros((C1, n2), F32)
    for pair in pairs_of(own_z):
        gs = shifted(p_ref, pair)
        both = jnp.concatenate([shifted(q_ref, pair), gs], axis=0)
        u = window(a_ref, pair)
        m_most = m_most + lax.dot_general(both, u[:cut], NT, preferred_element_type=F32)
        m_rest = m_rest + lax.dot_general(u[cut:], both, NT, preferred_element_type=F32)
        u = window(ta_ref, pair)
        n_most = n_most + lax.dot_general(gs, u[:cut], NT, preferred_element_type=F32)
        n_rest = n_rest + lax.dot_general(u[cut:], gs, NT, preferred_element_type=F32)
    for ref, most, rest in (
        (mb_ref, m_most[:n2] + n_most, m_rest[:, :n2] + n_rest),
        (ms_ref, m_most[n2:], m_rest[:, n2:]),
    ):
        rest = rest.T
        for c in range(3):
            rows = [most[c * C2 + q * part : c * C2 + (q + 1) * part] for q in range(Q)]
            for t in range(8):
                cols = slice(128 * (t // 4), 128 * (t // 4) + 128)
                ref[3 * t + c] = lanes_from([rolled(u[:, cols], C1 * (q - t % 4)) for q, u in enumerate(rows)], C1)
            rows = [rest[c * C2 + q * part : c * C2 + (q + 1) * part] for q in range(Q)]
            ref[24 + c] = jnp.concatenate(rows, axis=1)

    def wait_many(buf, count, sem):
        part = buf.at[pl.ds(0, count)]
        pltpu.make_async_copy(part, part, sem).wait()

    wait_many(pools, n_all - 1, pool_recv)
    for r in range(1, n_dp):
        to_partner(r).wait_recv()

    hd = jnp.zeros((outs, C2), F32)
    dpool = jnp.zeros((1, C2), F32)
    tdpool = jnp.zeros((1, C2), F32)
    group = n_x * n_y
    for d in range(n_dp):
        pair = jnp.sum(pools[d * group : (d + 1) * group], axis=0) / total_cells
        pooled, tpooled = pair[:, :C2], pair[:, C2:]
        out = jnp.sum(hw * pooled, axis=1, keepdims=True) + hb
        tout = jnp.sum(hw * tpooled + dh * pooled, axis=1, keepdims=True)
        dy = (out - column_of(tgts[d], small)) / batch
        tdy = tout / batch
        hd = hd + (tpooled * dy + pooled * tdy)
        dp = jnp.sum(dy * hw, axis=0, keepdims=True) / total_cells
        tdp = jnp.sum(tdy * hw + dy * dh, axis=0, keepdims=True) / total_cells
        dpool = jnp.where(me_d == d, dp, dpool)
        tdpool = jnp.where(me_d == d, tdp, tdpool)

    dcol, tcol = column_of(dpool, square), column_of(tdpool, square)

    def tile_of(column):
        return lanes_from(
            [jnp.broadcast_to(column[q * part : (q + 1) * part], (part, Q * C1)) for q in range(Q)], C1
        )

    dtile, ttile = tile_of(dcol), tile_of(tcol)
    owners = hs.shape[0]
    early = 27 // per

    def part_to(j):
        return remote(hs.at[j], rs.at[me], rs_send, rs_recv, coords(j * stride))

    def put(piece, block):
        at = piece % per * PIECE
        hs[piece // per, at : at + PIECE] = block.astype(BF16)

    def send_parts(first, last):
        for j in range(first, last):
            @pl.when(me != j * stride)
            def _():
                part_to(j).start()

    quad = jnp.zeros((PIECE, 128), F32)
    for k in range(27):
        term = mb_ref[k] * dtile + ms_ref[k] * ttile
        put(k, term)
        quad = quad + term * d2_ref[k]
    send_parts(0, early)

    for x, y in box(0, nx + 2, 0, ny + 2):
        slope = p_ref[x, y]
        g_ref[x, y] = (slope * dcol).astype(BF16)
        tg_ref[x, y] = (q_ref[x, y] * dcol + slope * tcol).astype(BF16)

    n1 = 3 * C1
    h1 = jnp.zeros((C1, 9 * ROWS), F32)
    for pair in pairs_of(box(0, nx, 0, ny)):
        end = jnp.concatenate([window(g_ref, pair, back[8:]), window(tg_ref, pair, back[8:])], axis=0)
        res = jnp.dot(lb_ref[...], window(g_ref, pair, back[:8]), preferred_element_type=F32)
        res = res + jnp.dot(lbr_ref[...], end, preferred_element_type=F32)
        tres = jnp.dot(lb_ref[:n1], window(tg_ref, pair, back[:8]), preferred_element_type=F32)
        tres = res[n1:] + tres
        grads = []
        for k, (x, y) in enumerate(pair):
            da = gathered(res[:n1, k * lanes : (k + 1) * lanes], C1)
            tda = gathered(tres[:, k * lanes : (k + 1) * lanes], C1)
            field_ref[:, x, y, :] = tda * total_cells
            grads.append((d_ref[1, x, y] * da + d_ref[0, x, y] * tda).astype(BF16))
        around = [(x + 2, y + 2) for x, y in pair]
        h1 = h1 + lax.dot_general(
            jnp.concatenate(grads, axis=1), window(v16, around), NT, preferred_element_type=F32
        )
    own1 = jnp.sum(d1 * h1, axis=0, keepdims=True)
    tail1 = jnp.concatenate([own1[:, 128:], jnp.zeros((1, 256 - 9 * ROWS), F32)], axis=1)
    quad = jnp.sum(quad, axis=0, keepdims=True) + own1[:, :128] + tail1
    quad_src[...] = quad
    wide = lax.dot_general(fold, h1.astype(BF16), (((0,), (0,)), ((), ())), preferred_element_type=F32)
    wide = jnp.where(match, wide, 0.0).astype(BF16)
    flat = lax.dot_general(spread, wide, NT, preferred_element_type=F32)
    for k in range(27, owners * per):
        put(k, flat[(k - 27) * PIECE : (k - 26) * PIECE] if k < 29 else jnp.zeros((PIECE, 128), F32))
    send_parts(early, owners)

    def quad_to(where):
        return remote(quad_src, quads.at[me], quad_send, quad_recv, where)

    each_other(lambda where: quad_to(where).start())
    quads[me] = quad

    hd_ref[...] = moved_rows(hd, outside_rows)

    def head_row(u):
        return jnp.concatenate([jnp.sum(u, axis=0, keepdims=True), jnp.zeros((1, 128 - C2), F32)], axis=1)


    slot = me // stride
    is_owner = lax.rem(me, stride) == 0
    if owners * stride != n_all:
        is_owner = is_owner & (slot < owners)

    def total_to(where):
        return remote(ag_src, h_ref.at[slot], ag_send, ag_recv, where)

    def own():
        wait_many(rs, n_all - 1, rs_recv)
        rs[me] = hs[slot]
        terms = [rs[k].astype(F32) for k in range(n_all)]
        while len(terms) > 1:
            terms = [sum(terms[k : k + 2]) for k in range(0, len(terms), 2)]
        mine = terms[0].astype(BF16)
        ag_src[...] = mine
        each_other(lambda where: total_to(where).start())
        h_ref[slot] = mine
        wait_many(h_ref, owners - 1, ag_recv)
        wait_many(hs, owners - 1, rs_send)
        wait_many(rs, n_all - 1, ag_send)

    def rest_of():
        wait_many(h_ref, owners, ag_recv)
        wait_many(hs, owners, rs_send)

    if owners == n_all:
        own()
    else:
        pl.when(is_owner)(own)
        pl.when(jnp.logical_not(is_owner))(rest_of)

    for k, (dx, dy, *_) in enumerate(moves):
        @pl.when(inside(dx, dy))
        def _():
            halo(k).wait_send()

    for r in range(1, n_dp):
        to_partner(r).wait_send()
    wait_many(pools, n_all - 1, pool_send)
    wait_many(quads, n_all - 1, quad_recv)
    wait_many(quads, n_all - 1, quad_send)
    quad_ref[0:1, :] = jnp.sum(quads[...], axis=0) + head_row(dh * hd)
    quad_ref[1:2, :] = head_row(dh * dh)


def last_kernel(
    per, h_ref, hd_ref, quad_ref, field_in, dir1_ref, dir2_ref,
    next1_ref, next2_ref, head_ref, ray_ref, field_out, sem,
):
    copy = pltpu.make_async_copy(field_in, field_out, sem)
    copy.start()
    h = h_ref[...].astype(F32).reshape(-1, 128)
    h1 = h[27 * PIECE : 27 * PIECE + 27]
    hd = hd_ref[...]
    dir1 = dir1_ref[...]
    rows = [h[k * PIECE : (k + 1) * PIECE].reshape(1, PIECE * 128) for k in range(27)]
    h2 = jnp.concatenate(rows, axis=0)
    dir2 = dir2_ref[...]

    def total(u):
        u = jnp.sum(u, axis=0, keepdims=True)
        return u if u.shape[1] == 128 else sum(u[:, j : j + 128] for j in range(0, u.shape[1], 128))

    def across(u):
        return jnp.sum(u, axis=1, keepdims=True)

    quad = across(quad_ref[0:1, :])
    length = across(total(dir1 * dir1) + total(dir2 * dir2) + quad_ref[1:2, :])
    head = jnp.sum(hd * hd, axis=0, keepdims=True)
    nrm = jnp.sqrt(across(total(h1 * h1) + total(h2 * h2)) + across(head) + 1e-06)
    scale = 1.0 / nrm
    next1_ref[...] = h1 * scale
    next2_ref[...] = h2 * scale
    head_ref[...] = hd * scale
    ray_ref[...] = quad / length
    copy.wait()


def per_device(
    volume, targets, conv1_w, conv1_b, conv2_w, conv2_b, head_w, head_b, dir1, dir2, dir_head
):
    nx, ny, lanes = volume.shape[2:]
    counts = tuple(lax.axis_size(name) for name in AXES)
    n_all = counts[0] * counts[1] * counts[2]
    total_cells = nx * counts[1] * ny * counts[2] * lanes
    batch = volume.shape[0] * counts[0]
    outs = head_w.shape[1]
    per = max(1, -(-29 // n_all))
    owners = -(-29 // per)
    stride = n_all // owners
    rounds = max(1, counts[1] - 1 - len(steps_out(nx)), counts[2] - 1 - len(steps_out(ny)))
    n_moves = len(spans(nx)) * len(spans(ny)) - 1
    shape = jax.ShapeDtypeStruct
    dma = pltpu.SemaphoreType.DMA
    hbm = pl.BlockSpec(memory_space=pltpu.HBM)
    args = (
        volume[0], targets, conv1_w, conv1_b[None], conv2_w, conv2_b[None], head_w.T, head_b[None], dir1, dir2, dir_head.T
    )

    args = tuple(pltpu.with_memory_space_constraint(a, pltpu.HBM) for a in args)

    def kernel(*refs):
        step_kernel(counts, total_cells, batch, stride, per, *refs)

    h, hd, quad, field = pl.pallas_call(
        kernel,
        in_specs=[hbm] * len(args),
        out_shape=(
            shape((owners, per * PIECE, 128), BF16),
            shape((outs, C2), F32),
            shape((2, 128), F32),
            shape((C1, nx, ny, lanes), F32),
        ),
        scratch_shapes=[pltpu.VMEM(a.shape, a.dtype) for a in args]
        + [
            pltpu.VMEM((nx + 6, ny + 6, C0, lanes), BF16),
            pltpu.VMEM((nx + 6, ny + 6, ROWS, lanes), BF16),
            pltpu.VMEM((nx + 4, ny + 4, C1, lanes), BF16),
            pltpu.VMEM((nx + 4, ny + 4, C1, lanes), BF16),
            pltpu.VMEM((2, nx, ny, C1, lanes), F32),
            pltpu.VMEM((nx + 2, ny + 2, C2, lanes), F32),
            pltpu.VMEM((nx + 2, ny + 2, C2, lanes), F32),
            pltpu.VMEM((nx + 2, ny + 2, C2, lanes), BF16),
            pltpu.VMEM((nx + 2, ny + 2, C2, lanes), BF16),
            pltpu.VMEM((6 * C2, 9 * C1), BF16),
            pltpu.VMEM((6 * C1, 8 * C2), BF16),
            pltpu.VMEM((6 * C2, 2 * C1), BF16),
            pltpu.VMEM((6 * C1, 2 * C2), BF16),
            pltpu.VMEM((27, PIECE, 128), F32),
            pltpu.VMEM((27, PIECE, 128), F32),
            pltpu.VMEM((27, PIECE, 128), F32),
            pltpu.VMEM((1, 128), F32),
            pltpu.VMEM((n_all, 1, 128), F32),
            pltpu.VMEM((1, 2 * C2), F32),
            pltpu.VMEM((n_all, 1, 2 * C2), F32),
            pltpu.VMEM((counts[0], 1, outs), F32),
            pltpu.VMEM((owners, per * PIECE, 128), BF16),
            pltpu.VMEM((n_all, per * PIECE, 128), BF16),
            pltpu.VMEM((per * PIECE, 128), BF16),
            dma((len(args),)), dma((n_moves,)), dma((n_moves,)), dma, dma, dma((counts[0],)), dma((counts[0],)),
            dma, dma, dma, dma, dma, dma, pltpu.SemaphoreType.REGULAR((rounds,)),
        ],
        compiler_params=pltpu.CompilerParams(
            collective_id=0, has_side_effects=True, vmem_limit_bytes=VMEM_LIMIT
        ),
    )(*args)

    def last(*refs):
        last_kernel(per, *refs)

    vmem = pl.BlockSpec(memory_space=pltpu.VMEM)
    next1, next2, head, ray, field = pl.pallas_call(
        last,
        in_specs=[vmem] * 6,
        out_specs=(vmem, vmem, vmem, vmem, hbm),
        out_shape=(
            shape(dir1.shape, F32), shape(dir2.shape, F32), shape((outs, C2), F32), shape((1, 1), F32),
            shape(field.shape, F32),
        ),
        scratch_shapes=[dma],
        compiler_params=pltpu.CompilerParams(vmem_limit_bytes=VMEM_LIMIT),
    )(h, hd, quad, field, dir1, dir2)
    return (next1, next2, head.T, ray[0, 0], field[None])


def solution(mesh):
    return jax.shard_map(
        per_device,
        mesh=mesh,
        in_specs=(P("dp", None, "gx", "gy", None), P("dp", None)) + (P(),) * 9,
        out_specs=(P(), P(), P(), P(), P("dp", None, "gx", "gy", None)),
        check_vma=False,
    )
```

```python
import jax
import jax.numpy as jnp
from jax import lax
from jax.experimental import pallas as pl
from jax.experimental.pallas import tpu as pltpu
from jax.sharding import PartitionSpec as P

C0 = 4
C1 = 32
C2 = 64
ROWS = 16
REACH = 3
PIECE = 16
Q = 4
VMEM_LIMIT = 24 * 1024 * 1024
F32 = jnp.float32
BF16 = jnp.bfloat16
MESH = pl.DeviceIdType.MESH
NT = (((1,), (1,)), ((), ()))
AXES = ("dp", "gx", "gy")


def silu_parts(z):
    s = 0.5 * jnp.tanh(0.5 * z) + 0.5
    act = z * s
    u = 1.0 - s
    return (act, s + act * u, s * u * ((2.0 + z) - (act + act)))


def window(ref, cells, taps=range(9)):
    columns = []
    for x, y in cells:
        columns.append(jnp.concatenate([ref[x + tap // 3, y + tap % 3] for tap in taps], axis=0))
    return jnp.concatenate(columns, axis=1)


def iota(shape, dim):
    return lax.broadcasted_iota(jnp.int32, shape, dim)


def channel_pick(rows_inside):
    inside = iota((C2, C2), 0 if rows_inside else 1)
    o = iota((C2, C2), 1 if rows_inside else 0)
    return inside == (o % Q) * (C2 // Q) + o // Q


def column_of(row, pick):
    return jnp.sum(jnp.where(pick, row, 0.0), axis=1, keepdims=True)


def row_of(column, pick):
    return jnp.sum(jnp.where(pick, column, 0.0), axis=0, keepdims=True)


def lanes_from(blocks, width):
    lane = iota(blocks[0].shape, 1)
    out = blocks[-1]
    for j in range(len(blocks) - 2, -1, -1):
        out = jnp.where(lane < (j + 1) * width, blocks[j], out)
    return out


def rolled(u, amount):
    amount %= u.shape[1]
    return pltpu.roll(u, amount, 1) if amount else u


def first_tables():
    wide = 9 * ROWS
    k = iota((32, wide), 0)
    col = iota((32, wide), 1)
    place = (col % ROWS) // C0
    c = jnp.where(place == 0, 1, jnp.where(place == 1, 0, 2))
    spread = jnp.where((place < 3) & (k == 3 * (col // ROWS) + c), 1.0, 0.0).astype(BF16)
    match = (iota((C0 * C1, wide), 0) % C0) == (iota((C0 * C1, wide), 1) % C0)
    fold = jnp.where(iota((C1, C0 * C1), 1) // C0 == iota((C1, C0 * C1), 0), 1.0, 0.0).astype(BF16)
    return spread, match, fold


def lane_of(shape):
    return lax.broadcasted_iota(jnp.int32, shape, len(shape) - 1)


def from_left(u):
    return jnp.where(lane_of(u.shape) == 0, 0.0, pltpu.roll(u, 1, 1))


def from_right(u):
    last = u.shape[1] - 1
    return jnp.where(lane_of(u.shape) == last, 0.0, pltpu.roll(u, last, 1))


def gathered(y, n):
    return from_left(y[:n]) + y[n : 2 * n] + from_right(y[2 * n : 3 * n])


def shifted(ref, cells):
    columns = []
    for x, y in cells:
        u = ref[x, y]
        columns.append(jnp.concatenate([from_right(u), u, from_left(u)], axis=0).astype(BF16))
    return jnp.concatenate(columns, axis=1)


def steps_out(size):
    found = []
    left = REACH
    while left > 0:
        found.append((len(found) + 1, min(size, left)))
        left -= size
    return found


def spans(size):
    found = [(0, 0, REACH, size)]
    for far, count in steps_out(size):
        found.append((far, size - count, REACH - (far - 1) * size - count, count))
        found.append((-far, 0, REACH + far * size, count))
    return found


def pairs_of(cells):
    return [cells[k : k + 2] for k in range(0, len(cells), 2)]


def step_kernel(
    counts, total_cells, batch, middle, per,
    v_hbm, tgt_hbm, w1_hbm, b1_hbm, w2_hbm, b2_hbm, hw_hbm, hb_hbm, k1_hbm, k2_hbm, dh_hbm,
    h_ref, hd_ref, quad_ref, field_ref,
    vin, tgt, w1, b1_in, w2, b2_in, hw_in, hb_in, k1, k2, dh_in,
    vraw, v16, a_ref, ta_ref, d_ref, p_ref, q_ref, g_ref, tg_ref, l2_ref, lb_ref, l2r_ref, lbr_ref, mb_ref, ms_ref, d2_ref,
    quad_src, quads, pool_src, pools, tgts, hs, rs, ag_src,
    in_sem, v_send, v_recv, pool_send, pool_recv, tgt_send, tgt_recv, rs_send, rs_recv, ag_send, ag_recv, quad_send, quad_recv, round_sem,
):
    n_dp, n_x, n_y = counts
    n_all = n_dp * n_x * n_y
    _, nx, ny, lanes = vin.shape
    loads = [
        pltpu.make_async_copy(src, dst, in_sem.at[k])
        for k, (src, dst) in enumerate(
            (
                (v_hbm, vin), (w2_hbm, w2), (k2_hbm, k2), (w1_hbm, w1), (k1_hbm, k1), (tgt_hbm, tgt),
                (b1_hbm, b1_in), (b2_hbm, b2_in), (hw_hbm, hw_in), (hb_hbm, hb_in), (dh_hbm, dh_in),
            )
        )
    ]
    me_d, me_x, me_y = [lax.axis_index(name) for name in AXES]
    me = (me_d * n_x + me_x) * n_y + me_y

    def coords(flat):
        return (flat // (n_x * n_y), lax.rem(flat // n_y, n_x), lax.rem(flat, n_y))

    def ring(at, count):
        after = [at]
        for k in range(1, count):
            after.append(jnp.where(at + k >= count, at + k - count, at + k))
        return after[1:] + after[:1]

    rings = ring(me_d, n_dp), ring(me_x, n_x), ring(me_y, n_y)

    def each_other(body):
        if n_all <= 32:
            everyone = [(d, x, y) for y in rings[2] for x in rings[1] for d in rings[0]]
            for where in everyone[:-1]:
                body(where)
        else:
            lax.fori_loop(1, n_all, lambda r, c: (body(coords(lax.rem(me + r, n_all))), c)[1], 0)

    barrier = pltpu.get_barrier_semaphore()
    reach_x, reach_y = len(steps_out(nx)), len(steps_out(ny))
    rounds = round_sem.shape[0]

    def inside(dx, dy):
        x, y = me_x + dx, me_y + dy
        return (x >= 0) & (x < n_x) & (y >= 0) & (y < n_y)

    def held(at, count, reach):
        return jnp.minimum(at, reach) + jnp.minimum(count - 1 - at, reach) + 1

    def tell(sem, far_x, far_y, cores):
        for dx in range(-far_x, far_x + 1):
            for dy in range(-far_y, far_y + 1):
                if dx or dy:
                    @pl.when(inside(dx, dy))
                    def _():
                        for d in cores:
                            pl.semaphore_signal(
                                sem, inc=1, device_id=(d, me_x + dx, me_y + dy), device_id_type=MESH
                            )
        for d in cores[:-1]:
            pl.semaphore_signal(sem, inc=1, device_id=(d, me_x, me_y), device_id_type=MESH)

    def tell_round(k):
        tell(round_sem.at[k], 1, 1, [me_d])

    def hear_round(k):
        pl.semaphore_wait(round_sem.at[k], held(me_x, n_x, 1) * held(me_y, n_y, 1) - 1)

    tell(barrier, reach_x, reach_y, rings[0])

    def remote(src, dst, send, recv, where):
        return pltpu.make_async_remote_copy(
            src_ref=src, dst_ref=dst, send_sem=send, recv_sem=recv, device_id=where, device_id_type=MESH
        )

    for load in loads:
        load.start()
    loads[0].wait()
    for x in range(nx):
        planes = [vin[c, x].astype(F32) for c in range(C0)]
        for y in range(ny):
            vraw[REACH + x, REACH + y] = jnp.concatenate([u[y : y + 1] for u in planes], axis=0).astype(BF16)
    for load in loads[1:]:
        load.wait()

    part = C2 // Q
    lane = iota((part, Q * C1), 1)
    for kind, ref in enumerate((w2, k2)):
        for c in range(3):
            for g in range(3):
                taps = range(4 * g, min(4 * g + 4, 9))
                rows = [ref[3 * t + c : 3 * t + c + 1, :].astype(F32).reshape(part, Q * C1) for t in taps]
                if kind:
                    for t, u in zip(taps, rows):
                        d2_ref[3 * t + c] = u
                for q in range(Q):
                    block = lanes_from([rolled(u, C1 * (j - q)) for j, u in enumerate(rows)], C1)
                    at = (kind * 3 + c) * C2 + q * part
                    if len(rows) == 1:
                        if kind == 0:
                            beside = rolled(rows[0], C1 - C1 * q)
                            l2r_ref[at : at + part] = jnp.where(lane < C1, block, 0.0)[:, : 2 * C1].astype(BF16)
                            l2r_ref[at + 3 * C2 : at + 3 * C2 + part] = beside[:, : 2 * C1].astype(BF16)
                        block = block[:, :C1]
                        if kind == 1:
                            l2r_ref[at : at + part, :C1] = block.astype(BF16)
                    l2_ref[at : at + part, 4 * g * C1 : 4 * g * C1 + block.shape[1]] = block.astype(BF16)

    pl.semaphore_wait(barrier, n_dp * held(me_x, n_x, reach_x) * held(me_y, n_y, reach_y) - 1)

    moves = []
    for dx, sx, tx, cx in spans(nx):
        for dy, sy, ty, cy in spans(ny):
            if dx or dy:
                moves.append((dx, dy, sx, tx, cx, sy, ty, cy))

    def halo(k):
        dx, dy, sx, tx, cx, sy, ty, cy = moves[k]
        return remote(
            vraw.at[pl.ds(REACH + sx, cx), pl.ds(REACH + sy, cy)], vraw.at[pl.ds(tx, cx), pl.ds(ty, cy)],
            v_send.at[k], v_recv.at[k], (me_d, me_x + dx, me_y + dy),
        )

    for k, (dx, dy, *_) in enumerate(moves):
        @pl.when(inside(dx, dy))
        def _():
            halo(k).start()

    def to_partner(r):
        other = lax.rem(me_d + r, n_dp)
        return remote(tgt, tgts.at[me_d], tgt_send.at[r], tgt_recv.at[r], (other, me_x, me_y))

    for r in range(1, n_dp):
        to_partner(r).start()
    tgts[me_d] = tgt[...]
    tell_round(0)

    for kind in range(2):
        for c in range(3):
            rows = l2_ref[(kind * 3 + c) * C2 : (kind * 3 + c + 1) * C2, :].astype(F32)
            at = (kind * 3 + 2 - c) * C1
            both = jnp.concatenate([rows[:, :128], rows[:, 128:256]], axis=0).T
            for m in range(4):
                lb_ref[at : at + C1, 128 * m : 128 * m + 128] = both[C1 * m : C1 * m + C1].astype(BF16)
            end = rows[:, 256:].T.astype(BF16)
            none = jnp.zeros((C1, C2), BF16)
            if kind == 0:
                lbr_ref[at : at + C1] = jnp.concatenate([end, none], axis=1)
                lbr_ref[at + 3 * C1 : at + 4 * C1] = jnp.concatenate([none, end], axis=1)
            else:
                lbr_ref[at : at + C1, :C2] = end
    back = [8 - t for t in (0, 4, 1, 5, 2, 6, 3, 7, 8)]

    spread, match, fold = first_tables()
    l1 = []
    high = k1[...].astype(BF16)
    for flat in (w1[...], high, (k1[...] - high.astype(F32)).astype(BF16)):
        flat = jnp.concatenate([flat.astype(F32), jnp.zeros((5, C0 * C1), F32)], axis=0)
        wide = jnp.dot(flat.T.astype(BF16), spread, preferred_element_type=F32)
        wide = jnp.where(match, wide, 0.0).astype(BF16)
        l1.append(jnp.dot(fold, wide, preferred_element_type=F32))
    d1 = l1[1] + l1[2]
    l1 = jnp.concatenate(l1[:2], axis=0).astype(BF16)
    b1 = column_of(b1_in[...], iota((C1, C1), 0) == iota((C1, C1), 1))
    inside_rows = channel_pick(True)
    outside_rows = channel_pick(False)
    b2 = column_of(b2_in[...], inside_rows)
    outs = hw_in.shape[0]
    square = iota((C2, C2), 0) == iota((C2, C2), 1)

    def moved_rows(whole, pick):
        return jnp.concatenate(
            [row_of(column_of(whole[m : m + 1], pick), square) for m in range(outs)], axis=0
        )

    def head_rows(ref):
        return moved_rows(ref[...], inside_rows)

    hw, dh = head_rows(hw_in), head_rows(dh_in)
    small = iota((outs, outs), 0) == iota((outs, outs), 1)
    hb = column_of(hb_in[...], small)

    def arrive(near):
        for k, (dx, dy, sx, tx, cx, sy, ty, cy) in enumerate(moves):
            if (abs(dx) <= 1 and abs(dy) <= 1) == near:
                came = inside(-dx, -dy)

                @pl.when(came)
                def _():
                    halo(k).wait_recv()

                @pl.when(jnp.logical_not(came))
                def _():
                    vraw[tx : tx + cx, ty : ty + cy] = jnp.zeros((cx, cy, C0, lanes), BF16)

    sub = iota((8, lanes), 0)

    def expand(cells):
        for x, y in cells:
            u = vraw[x, y].astype(F32)
            full = jnp.concatenate([u, u], axis=0)
            top = jnp.where(sub < C0, full, from_left(full))
            low = jnp.where(sub < C0, from_right(full), 0.0)
            v16[x, y] = jnp.concatenate([top, low], axis=0).astype(BF16)

    def valid(x, y):
        gx, gy = me_x * nx + x, me_y * ny + y
        return jnp.where((gx >= 0) & (gx < n_x * nx) & (gy >= 0) & (gy < n_y * ny), 1.0, 0.0).astype(F32)

    def first_block(cells):
        for pair in pairs_of(cells):
            res = jnp.dot(l1, window(v16, pair), preferred_element_type=F32)
            for k, (x, y) in enumerate(pair):
                part = res[:, k * lanes : (k + 1) * lanes]
                t1 = part[C1:]
                act, slope, bend = silu_parts(part[:C1] + b1)
                mine = 2 <= x < nx + 2 and 2 <= y < ny + 2
                if mine:
                    a_ref[x, y] = act.astype(BF16)
                    ta_ref[x, y] = (slope * t1).astype(BF16)
                    d_ref[0, x - 2, y - 2] = slope
                    d_ref[1, x - 2, y - 2] = bend * t1
                else:
                    mask = valid(x - 2, y - 2)
                    a_ref[x, y] = (act * mask).astype(BF16)
                    ta_ref[x, y] = (slope * t1 * mask).astype(BF16)

    n2 = 3 * C2

    def second_block(cells, sums):
        for pair in pairs_of(cells):
            end = jnp.concatenate([window(a_ref, pair, (8,)), window(ta_ref, pair, (8,))], axis=0)
            res = jnp.dot(l2_ref[:, : 8 * C1], window(a_ref, pair, range(8)), preferred_element_type=F32)
            res = res + jnp.dot(l2r_ref[...], end, preferred_element_type=F32)
            tres = jnp.dot(l2_ref[:n2, : 8 * C1], window(ta_ref, pair, range(8)), preferred_element_type=F32)
            tres = res[n2:] + tres
            for k, (x, y) in enumerate(pair):
                z2 = gathered(res[:n2, k * lanes : (k + 1) * lanes], C2) + b2
                t2 = gathered(tres[:, k * lanes : (k + 1) * lanes], C2)
                act, slope, bend = silu_parts(z2)
                if sums is not None:
                    sums = (sums[0] + act, sums[1] + slope * t2)
                    p_ref[x, y] = slope
                    q_ref[x, y] = bend * t2
                else:
                    mask = valid(x - 1, y - 1)
                    p_ref[x, y] = slope * mask
                    q_ref[x, y] = bend * t2 * mask
        return sums

    def box(x0, x1, y0, y1):
        return [(x, y) for x in range(x0, x1) for y in range(y0, y1)]

    near_v = box(1, nx + 5, 1, ny + 5)
    far_v = [c for c in box(0, nx + 6, 0, ny + 6) if c not in near_v]
    near_a = box(1, nx + 3, 1, ny + 3)
    far_a = [c for c in box(0, nx + 4, 0, ny + 4) if c not in near_a]
    own_z = box(1, nx + 1, 1, ny + 1)
    far_z = [c for c in box(0, nx + 2, 0, ny + 2) if c not in own_z]

    for k in range(rounds - 1):
        hear_round(k)
        tell_round(k + 1)
    arrive(True)
    expand(near_v)
    first_block(near_a)
    zero = jnp.zeros((C2, lanes), F32)
    sums = second_block(own_z, (zero, zero))
    row = jnp.sum(jnp.concatenate(sums, axis=0).T, axis=0, keepdims=True)
    pool_src[...] = row

    def pool_to(where):
        return remote(pool_src, pools.at[me], pool_send, pool_recv, where)

    hear_round(rounds - 1)
    each_other(lambda where: pool_to(where).start())
    pools[me] = row

    arrive(False)
    expand(far_v)
    first_block(far_a)
    second_block(far_z, None)

    cut = 8 * C1
    m_most = jnp.zeros((2 * n2, cut), F32)
    m_rest = jnp.zeros((C1, 2 * n2), F32)
    n_most = jnp.zeros((n2, cut), F32)
    n_rest = jnp.zeros((C1, n2), F32)
    for pair in pairs_of(own_z):
        gs = shifted(p_ref, pair)
        both = jnp.concatenate([shifted(q_ref, pair), gs], axis=0)
        u = window(a_ref, pair)
        m_most = m_most + lax.dot_general(both, u[:cut], NT, preferred_element_type=F32)
        m_rest = m_rest + lax.dot_general(u[cut:], both, NT, preferred_element_type=F32)
        u = window(ta_ref, pair)
        n_most = n_most + lax.dot_general(gs, u[:cut], NT, preferred_element_type=F32)
        n_rest = n_rest + lax.dot_general(u[cut:], gs, NT, preferred_element_type=F32)
    for ref, most, rest in (
        (mb_ref, m_most[:n2] + n_most, m_rest[:, :n2] + n_rest),
        (ms_ref, m_most[n2:], m_rest[:, n2:]),
    ):
        rest = rest.T
        for c in range(3):
            rows = [most[c * C2 + q * part : c * C2 + (q + 1) * part] for q in range(Q)]
            for t in range(8):
                cols = slice(128 * (t // 4), 128 * (t // 4) + 128)
                ref[3 * t + c] = lanes_from([rolled(u[:, cols], C1 * (q - t % 4)) for q, u in enumerate(rows)], C1)
            rows = [rest[c * C2 + q * part : c * C2 + (q + 1) * part] for q in range(Q)]
            ref[24 + c] = jnp.concatenate(rows, axis=1)

    def wait_many(buf, count, sem):
        part = buf.at[pl.ds(0, count)]
        pltpu.make_async_copy(part, part, sem).wait()

    wait_many(pools, n_all - 1, pool_recv)
    for r in range(1, n_dp):
        to_partner(r).wait_recv()

    hd = jnp.zeros((outs, C2), F32)
    dpool = jnp.zeros((1, C2), F32)
    tdpool = jnp.zeros((1, C2), F32)
    group = n_x * n_y
    for d in range(n_dp):
        pair = jnp.sum(pools[d * group : (d + 1) * group], axis=0) / total_cells
        pooled, tpooled = pair[:, :C2], pair[:, C2:]
        out = jnp.sum(hw * pooled, axis=1, keepdims=True) + hb
        tout = jnp.sum(hw * tpooled + dh * pooled, axis=1, keepdims=True)
        dy = (out - column_of(tgts[d], small)) / batch
        tdy = tout / batch
        hd = hd + (tpooled * dy + pooled * tdy)
        dp = jnp.sum(dy * hw, axis=0, keepdims=True) / total_cells
        tdp = jnp.sum(tdy * hw + dy * dh, axis=0, keepdims=True) / total_cells
        dpool = jnp.where(me_d == d, dp, dpool)
        tdpool = jnp.where(me_d == d, tdp, tdpool)

    dcol, tcol = column_of(dpool, square), column_of(tdpool, square)

    def tile_of(column):
        return lanes_from(
            [jnp.broadcast_to(column[q * part : (q + 1) * part], (part, Q * C1)) for q in range(Q)], C1
        )

    dtile, ttile = tile_of(dcol), tile_of(tcol)
    owners = hs.shape[0]
    early = 27 // per

    y0, width = middle

    def owner_of(j):
        return (j // (n_x * width), j // width % n_x, y0 + j % width)

    def part_to(j):
        return remote(hs.at[j], rs.at[me], rs_send, rs_recv, owner_of(j))

    def put(piece, block):
        at = piece % per * PIECE
        hs[piece // per, at : at + PIECE] = block.astype(BF16)

    def send_parts(first, last):
        for j in range(first, last):
            d, x, y = owner_of(j)

            @pl.when(jnp.logical_not((me_d == d) & (me_x == x) & (me_y == y)))
            def _():
                part_to(j).start()

    quad = jnp.zeros((PIECE, 128), F32)
    for k in range(27):
        term = mb_ref[k] * dtile + ms_ref[k] * ttile
        put(k, term)
        quad = quad + term * d2_ref[k]
    send_parts(0, early)

    for x, y in box(0, nx + 2, 0, ny + 2):
        slope = p_ref[x, y]
        g_ref[x, y] = (slope * dcol).astype(BF16)
        tg_ref[x, y] = (q_ref[x, y] * dcol + slope * tcol).astype(BF16)

    n1 = 3 * C1
    h1 = jnp.zeros((C1, 9 * ROWS), F32)
    for pair in pairs_of(box(0, nx, 0, ny)):
        end = jnp.concatenate([window(g_ref, pair, back[8:]), window(tg_ref, pair, back[8:])], axis=0)
        res = jnp.dot(lb_ref[...], window(g_ref, pair, back[:8]), preferred_element_type=F32)
        res = res + jnp.dot(lbr_ref[...], end, preferred_element_type=F32)
        tres = jnp.dot(lb_ref[:n1], window(tg_ref, pair, back[:8]), preferred_element_type=F32)
        tres = res[n1:] + tres
        grads = []
        for k, (x, y) in enumerate(pair):
            da = gathered(res[:n1, k * lanes : (k + 1) * lanes], C1)
            tda = gathered(tres[:, k * lanes : (k + 1) * lanes], C1)
            field_ref[:, x, y, :] = tda * total_cells
            grads.append((d_ref[1, x, y] * da + d_ref[0, x, y] * tda).astype(BF16))
        around = [(x + 2, y + 2) for x, y in pair]
        h1 = h1 + lax.dot_general(
            jnp.concatenate(grads, axis=1), window(v16, around), NT, preferred_element_type=F32
        )
    own1 = jnp.sum(d1 * h1, axis=0, keepdims=True)
    tail1 = jnp.concatenate([own1[:, 128:], jnp.zeros((1, 256 - 9 * ROWS), F32)], axis=1)
    quad = jnp.sum(quad, axis=0, keepdims=True) + own1[:, :128] + tail1
    quad_src[...] = quad
    wide = lax.dot_general(fold, h1.astype(BF16), (((0,), (0,)), ((), ())), preferred_element_type=F32)
    wide = jnp.where(match, wide, 0.0).astype(BF16)
    flat = lax.dot_general(spread, wide, NT, preferred_element_type=F32)
    for k in range(27, owners * per):
        put(k, flat[(k - 27) * PIECE : (k - 26) * PIECE] if k < 29 else jnp.zeros((PIECE, 128), F32))
    send_parts(early, owners)

    def quad_to(where):
        return remote(quad_src, quads.at[me], quad_send, quad_recv, where)

    each_other(lambda where: quad_to(where).start())
    quads[me] = quad

    hd_ref[...] = moved_rows(hd, outside_rows)

    def head_row(u):
        return jnp.concatenate([jnp.sum(u, axis=0, keepdims=True), jnp.zeros((1, 128 - C2), F32)], axis=1)


    slot = (me_d * n_x + me_x) * width + me_y - y0
    is_owner = (me_y >= y0) & (me_y < y0 + width) & (slot < owners)

    def total_to(where):
        return remote(ag_src, h_ref.at[slot], ag_send, ag_recv, where)

    def own():
        wait_many(rs, n_all - 1, rs_recv)
        rs[me] = hs[slot]
        terms = [rs[k].astype(F32) for k in range(n_all)]
        while len(terms) > 1:
            terms = [sum(terms[k : k + 2]) for k in range(0, len(terms), 2)]
        mine = terms[0].astype(BF16)
        ag_src[...] = mine
        each_other(lambda where: total_to(where).start())
        h_ref[slot] = mine
        wait_many(h_ref, owners - 1, ag_recv)
        wait_many(hs, owners - 1, rs_send)
        wait_many(rs, n_all - 1, ag_send)

    def rest_of():
        wait_many(h_ref, owners, ag_recv)
        wait_many(hs, owners, rs_send)

    pl.when(is_owner)(own)
    pl.when(jnp.logical_not(is_owner))(rest_of)

    for k, (dx, dy, *_) in enumerate(moves):
        @pl.when(inside(dx, dy))
        def _():
            halo(k).wait_send()

    for r in range(1, n_dp):
        to_partner(r).wait_send()
    wait_many(pools, n_all - 1, pool_send)
    wait_many(quads, n_all - 1, quad_recv)
    wait_many(quads, n_all - 1, quad_send)
    quad_ref[0:1, :] = jnp.sum(quads[...], axis=0) + head_row(dh * hd)
    quad_ref[1:2, :] = head_row(dh * dh)


def last_kernel(
    per, h_ref, hd_ref, quad_ref, field_in, dir1_ref, dir2_ref,
    next1_ref, next2_ref, head_ref, ray_ref, field_out, sem,
):
    copy = pltpu.make_async_copy(field_in, field_out, sem)
    copy.start()
    h = h_ref[...].astype(F32).reshape(-1, 128)
    h1 = h[27 * PIECE : 27 * PIECE + 27]
    hd = hd_ref[...]
    dir1 = dir1_ref[...]
    rows = [h[k * PIECE : (k + 1) * PIECE].reshape(1, PIECE * 128) for k in range(27)]
    h2 = jnp.concatenate(rows, axis=0)
    dir2 = dir2_ref[...]

    def total(u):
        u = jnp.sum(u, axis=0, keepdims=True)
        return u if u.shape[1] == 128 else sum(u[:, j : j + 128] for j in range(0, u.shape[1], 128))

    def across(u):
        return jnp.sum(u, axis=1, keepdims=True)

    quad = across(quad_ref[0:1, :])
    length = across(total(dir1 * dir1) + total(dir2 * dir2) + quad_ref[1:2, :])
    head = jnp.sum(hd * hd, axis=0, keepdims=True)
    nrm = jnp.sqrt(across(total(h1 * h1) + total(h2 * h2)) + across(head) + 1e-06)
    scale = 1.0 / nrm
    next1_ref[...] = h1 * scale
    next2_ref[...] = h2 * scale
    head_ref[...] = hd * scale
    ray_ref[...] = quad / length
    copy.wait()


def per_device(
    volume, targets, conv1_w, conv1_b, conv2_w, conv2_b, head_w, head_b, dir1, dir2, dir_head
):
    nx, ny, lanes = volume.shape[2:]
    counts = tuple(lax.axis_size(name) for name in AXES)
    n_all = counts[0] * counts[1] * counts[2]
    total_cells = nx * counts[1] * ny * counts[2] * lanes
    batch = volume.shape[0] * counts[0]
    outs = head_w.shape[1]
    width = max(1, counts[2] // 2)
    middle = ((counts[2] - width) // 2, width)
    per = -(-29 // (counts[0] * counts[1] * width))
    owners = -(-29 // per)
    rounds = max(1, counts[1] - 1 - len(steps_out(nx)), counts[2] - 1 - len(steps_out(ny)))
    n_moves = len(spans(nx)) * len(spans(ny)) - 1
    shape = jax.ShapeDtypeStruct
    dma = pltpu.SemaphoreType.DMA
    hbm = pl.BlockSpec(memory_space=pltpu.HBM)
    args = (
        volume[0], targets, conv1_w, conv1_b[None], conv2_w, conv2_b[None], head_w.T, head_b[None], dir1, dir2, dir_head.T
    )

    args = tuple(pltpu.with_memory_space_constraint(a, pltpu.HBM) for a in args)

    def kernel(*refs):
        step_kernel(counts, total_cells, batch, middle, per, *refs)

    h, hd, quad, field = pl.pallas_call(
        kernel,
        in_specs=[hbm] * len(args),
        out_shape=(
            shape((owners, per * PIECE, 128), BF16),
            shape((outs, C2), F32),
            shape((2, 128), F32),
            shape((C1, nx, ny, lanes), F32),
        ),
        scratch_shapes=[pltpu.VMEM(a.shape, a.dtype) for a in args]
        + [
            pltpu.VMEM((nx + 6, ny + 6, C0, lanes), BF16),
            pltpu.VMEM((nx + 6, ny + 6, ROWS, lanes), BF16),
            pltpu.VMEM((nx + 4, ny + 4, C1, lanes), BF16),
            pltpu.VMEM((nx + 4, ny + 4, C1, lanes), BF16),
            pltpu.VMEM((2, nx, ny, C1, lanes), F32),
            pltpu.VMEM((nx + 2, ny + 2, C2, lanes), F32),
            pltpu.VMEM((nx + 2, ny + 2, C2, lanes), F32),
            pltpu.VMEM((nx + 2, ny + 2, C2, lanes), BF16),
            pltpu.VMEM((nx + 2, ny + 2, C2, lanes), BF16),
            pltpu.VMEM((6 * C2, 9 * C1), BF16),
            pltpu.VMEM((6 * C1, 8 * C2), BF16),
            pltpu.VMEM((6 * C2, 2 * C1), BF16),
            pltpu.VMEM((6 * C1, 2 * C2), BF16),
            pltpu.VMEM((27, PIECE, 128), F32),
            pltpu.VMEM((27, PIECE, 128), F32),
            pltpu.VMEM((27, PIECE, 128), F32),
            pltpu.VMEM((1, 128), F32),
            pltpu.VMEM((n_all, 1, 128), F32),
            pltpu.VMEM((1, 2 * C2), F32),
            pltpu.VMEM((n_all, 1, 2 * C2), F32),
            pltpu.VMEM((counts[0], 1, outs), F32),
            pltpu.VMEM((owners, per * PIECE, 128), BF16),
            pltpu.VMEM((n_all, per * PIECE, 128), BF16),
            pltpu.VMEM((per * PIECE, 128), BF16),
            dma((len(args),)), dma((n_moves,)), dma((n_moves,)), dma, dma, dma((counts[0],)), dma((counts[0],)),
            dma, dma, dma, dma, dma, dma, pltpu.SemaphoreType.REGULAR((rounds,)),
        ],
        compiler_params=pltpu.CompilerParams(
            collective_id=0, has_side_effects=True, vmem_limit_bytes=VMEM_LIMIT
        ),
    )(*args)

    def last(*refs):
        last_kernel(per, *refs)

    vmem = pl.BlockSpec(memory_space=pltpu.VMEM)
    next1, next2, head, ray, field = pl.pallas_call(
        last,
        in_specs=[vmem] * 6,
        out_specs=(vmem, vmem, vmem, vmem, hbm),
        out_shape=(
            shape(dir1.shape, F32), shape(dir2.shape, F32), shape((outs, C2), F32), shape((1, 1), F32),
            shape(field.shape, F32),
        ),
        scratch_shapes=[dma],
        compiler_params=pltpu.CompilerParams(vmem_limit_bytes=VMEM_LIMIT),
    )(h, hd, quad, field, dir1, dir2)
    return (next1, next2, head.T, ray[0, 0], field[None])


def solution(mesh):
    return jax.shard_map(
        per_device,
        mesh=mesh,
        in_specs=(P("dp", None, "gx", "gy", None), P("dp", None)) + (P(),) * 9,
        out_specs=(P(), P(), P(), P(), P("dp", None, "gx", "gy", None)),
        check_vma=False,
    )
```
